256 devices in a mesh: gx: 8 (over z), gy: 8 (over x, core), gz: 4 (over y).
Axes of the slice: x: 4, y: 4, z: 8, core: 2. Of those that a mesh axis runs over, the one named last changes fastest.
Arguments:
- element_state: float32 [9, 35, 32768], P(None, None, ('gx', 'gy', 'gz')), may hold values from -6 to 6
- jacobians: float32 [3, 9, 9, 32768], P(None, None, None, ('gx', 'gy', 'gz')), may hold values from -1.25 to 1.25
- stiffness: float32 [3, 35, 35], replicated, may hold values from -1 to 1
- projection: float32 [4, 15, 35], replicated, may hold values from -1 to 1
- flux_self: float32 [4, 9, 9, 32768], P(None, None, None, ('gx', 'gy', 'gz')), may hold values from -1 to 1
- flux_other: float32 [4, 9, 9, 32768], P(None, None, None, ('gx', 'gy', 'gz')), may hold values from -1 to 1
- face_source: int32 [4, 32768], P(None, ('gx', 'gy', 'gz')), may hold values from 0 to 607, as said below
- send_faces: int32 [6, 4096], P(None, ('gx', 'gy', 'gz')), may hold values from 0 to 511
- cluster_mask: int32 [32768], P(('gx', 'gy', 'gz')), may hold values from 0 to 1
- seafloor_face: int32 [2097152], P(('gx', 'gy', 'gz')), may hold values from -1 to 511, as said below
- ocean_cell: int32 [64, 4, 8192], P(('gx', 'gy')), may hold values from 0 to 65535
- ocean_weight: float32 [64, 4, 15, 8192], P(('gx', 'gy')), may hold values from 0 to 0.5
- height: float32 [2048, 2048], P('gx', 'gy'), may hold values from -6 to 6
- east_flow: float32 [2048, 2048], P('gx', 'gy'), may hold values from -6 to 6
- north_flow: float32 [2048, 2048], P('gx', 'gy'), may hold values from -6 to 6
- water_depth: float32 [2048, 2048], P('gx', 'gy'), may hold values from 0.5 to 2
Outputs:
- next_state: float32 [9, 35, 32768], P(None, None, ('gx', 'gy', 'gz'))
- new_height: float32 [2048, 2048], P('gx', 'gy')
- new_east: float32 [2048, 2048], P('gx', 'gy')
- new_north: float32 [2048, 2048], P('gx', 'gy')
The draws below stay inside these ranges and needn't reach their ends.
Inputs may be any that keep to these rules, and one draw needn't show every extreme that they name: `face_source`: within a partition, each of the 96 received columns (numbered from 512) is named by exactly one face; all other faces name the partition's own trace columns. `seafloor_face`: values are local face numbers or -1 for an empty slot. In each block of 128 slots of one partition for one tile the live slots come first and at least one is live; for one tile, the block of every partition is full.
All inputs are finite; a program needn't handle non-finite values.
Results may differ from the reference program's by a relative error of at most 0.0003.
Values sent between devices are 32-bit elements; how exact they have to be, the bound alone decides.
No kernel may reach another device: no remote copies, remote signals or barrier semaphores. Data moves between devices by JAX's collectives and lax.ppermute only.
A program may use at most 128 MiB of HBM per device.

```python
import math
import jax
import jax.numpy as jnp
from jax import lax

NQ = 9
NB = 35
NF = 15
E_DEV = 128
SLOTS = 128
CXO = 256
CYO = 256
BLOCK = 16
ELEMS = 32768
TILES = 64
NXO = 2048
NYO = 2048
N_GX = 8
N_GY = 8
N_GZ = 4
DEVICES = 256


def draw_face_source(key, part):
    partitions = ELEMS // E_DEV
    device_keys = jax.random.split(key, partitions)

    def per_device(single_key):
        key_rank, key_local = jax.random.split(single_key)
        order_rank = jax.random.permutation(key_rank, 4 * E_DEV).astype(jnp.int32)
        local_face = jax.random.randint(key_local, (4 * E_DEV,), 0, 4 * E_DEV)
        chosen = jnp.where(order_rank < 6 * BLOCK, 4 * E_DEV + order_rank, local_face)
        return chosen.reshape(4, E_DEV)
    stacked = jax.vmap(per_device)(device_keys)
    return jnp.transpose(stacked, (1, 0, 2)).reshape(4, ELEMS).astype(jnp.int32)


def draw_seafloor_face(key, part):
    partitions = ELEMS // E_DEV
    key_full, key_count, key_face = jax.random.split(jax.random.fold_in(key, 17), 3)
    full_tile = jax.random.randint(key_full, (), 0, TILES)
    live_count = jax.random.randint(key_count, (partitions, TILES, 1), 1, SLOTS + 1)
    tile_ids = jnp.arange(TILES, dtype=jnp.int32)[None, :, None]
    live_count = jnp.where(tile_ids == full_tile, SLOTS, live_count)
    face_ids = jax.random.randint(key_face, (partitions, TILES, SLOTS), 0, 4 * E_DEV)
    slot_ids = jnp.arange(SLOTS, dtype=jnp.int32)[None, None, :]
    live = slot_ids < live_count
    return jnp.where(live, face_ids, -1).reshape(-1).astype(jnp.int32)


def draw_cluster_mask(key, part):
    partitions = ELEMS // E_DEV
    key_level, key_draw = jax.random.split(key)
    levels = jax.random.randint(key_level, (partitions, 1), 2, 9)
    rolled = jax.random.randint(key_draw, (partitions, E_DEV), 0, 8)
    return (rolled < levels).astype(jnp.int32).reshape(-1)


def touch_ends(entries, stream_key, low, top_value):
    longest = entries.shape.index(max(entries.shape))
    spots = []
    for shift in (0, 1):
        where = [jax.random.randint(jax.random.fold_in(stream_key, axis), (), 0, length) for axis, length in enumerate(entries.shape)]
        where[longest] = (where[longest] + shift) % entries.shape[longest]
        spots.append(tuple(where))
    return entries.at[spots[0]].set(low).at[spots[1]].set(top_value)


def block_levels(key, dims, pieces, smallest, top_value):
    level, own = 1.0, jax.random.fold_in(key, 6)
    for dim, blocks in pieces:
        steps = jnp.exp(jax.random.uniform(jax.random.fold_in(own, dim), (blocks,), jnp.float32, smallest / len(pieces), top_value / len(pieces)))
        level = level * jnp.repeat(steps, dims[dim] // blocks).reshape([-1 if axis == dim else 1 for axis in range(len(dims))])
    return level


def centred(key, extent, spread, limit, cuts=(), kind=jnp.bfloat16):
    entries = spread * jax.random.normal(key, extent, jnp.float32)
    if cuts:
        entries = entries * block_levels(key, extent, cuts, -0.22, 0.18)
    return jnp.clip(entries, -limit, limit).astype(kind)


def setup_inputs(seed: int = 0) -> dict:
    keys = jax.random.split(jax.random.key(seed), 17)
    return {
        "element_state": centred(keys[0], (NQ, NB, ELEMS), 1.0, 6.0, ((2, 256),), jnp.float32),
        "jacobians": centred(keys[1], (3, NQ, NQ, ELEMS), (3 * NQ) ** -0.5, 1.25, ((3, 256),), jnp.float32),
        "stiffness": centred(keys[2], (3, NB, NB), NB ** -0.5, 1.0, (), jnp.float32),
        "projection": centred(keys[3], (4, NF, NB), NB ** -0.5, 1.0, (), jnp.float32),
        "flux_self": centred(keys[4], (4, NQ, NQ, ELEMS), (4 * NQ) ** -0.5, 1.0, ((3, 256),), jnp.float32),
        "flux_other": centred(keys[5], (4, NQ, NQ, ELEMS), (4 * NQ) ** -0.5, 1.0, ((3, 256),), jnp.float32),
        "face_source": draw_face_source(jax.random.fold_in(keys[16], 71), 0),
        "send_faces": touch_ends(jax.random.randint(keys[7], (6, BLOCK * DEVICES), 0, 4 * E_DEV), jax.random.fold_in(keys[7], 1), 0, (4 * E_DEV) - 1).astype(jnp.int32),
        "cluster_mask": draw_cluster_mask(jax.random.fold_in(keys[16], 71), 0),
        "seafloor_face": draw_seafloor_face(jax.random.fold_in(keys[16], 71), 0),
        "ocean_cell": touch_ends(jax.random.randint(keys[10], (TILES, N_GZ, TILES * SLOTS), 0, CXO * CYO), jax.random.fold_in(keys[10], 1), 0, (CXO * CYO) - 1).astype(jnp.int32),
        "ocean_weight": jnp.clip(0.5 * jax.random.uniform(keys[11], (TILES, N_GZ, NF, TILES * SLOTS), jnp.float32) ** block_levels(keys[11], (TILES, N_GZ, NF, TILES * SLOTS), ((0, 64),), -0.2, 0.2), 0.0, 0.5),
        "height": centred(keys[12], (NXO, NYO), 1.0, 6.0, ((0, 8), (1, 8)), jnp.float32),
        "east_flow": centred(keys[13], (NXO, NYO), 1.0, 6.0, ((0, 8), (1, 8)), jnp.float32),
        "north_flow": centred(keys[14], (NXO, NYO), 1.0, 6.0, ((0, 8), (1, 8)), jnp.float32),
        "water_depth": jnp.clip(jnp.exp(math.log(2.0) - 1.3862944 * jax.random.uniform(keys[15], (NXO, NYO), jnp.float32) ** block_levels(keys[15], (NXO, NYO), ((0, 8), (1, 8)), -0.2, 0.2)), 0.5, 2.0),
    }


time_step = 1.5
ocean_step = 0.5
highest = lax.Precision.HIGHEST


def derivative(dof_state, jacobian_local, stiffness):
    coupled = jnp.einsum('dpqe,qbe->dpbe', jacobian_local, dof_state, precision=highest)
    return -jnp.einsum('dcb,dpbe->pce', stiffness, coupled, precision=highest)


def predictor(dof_state, jacobian_local, stiffness):
    weight_now = time_step
    integral = weight_now * dof_state
    current = dof_state
    for degree in range(1, 5):
        current = derivative(current, jacobian_local, stiffness)
        weight_now = weight_now * time_step / (degree + 1)
        integral = integral + weight_now * current
    return integral


def volume_term(integral, jacobian_local, stiffness):
    coupled = jnp.einsum('dpqe,qbe->dpbe', jacobian_local, integral, precision=highest)
    return jnp.einsum('dbc,dpbe->pce', stiffness, coupled, precision=highest)


def trace_table(integral, projection):
    traces = jnp.einsum('fab,qbe->qafe', projection, integral, precision=highest)
    return traces.reshape(NQ * NF, 4 * integral.shape[2])


def flux_term(trace_flat, neighbour_table, face_source, flux_self, flux_other, projection):
    element_count = face_source.shape[1]
    own_traces = trace_flat.reshape(NQ, NF, 4, element_count)
    result = jnp.zeros((NQ, NB, element_count), jnp.float32)
    for side_index in range(4):
        remote = jnp.take(neighbour_table, face_source[side_index], axis=1).reshape(NQ, NF, element_count)
        numeric = jnp.einsum('qae,qpe->pae', own_traces[:, :, side_index], flux_self[side_index], precision=highest)
        numeric = numeric + jnp.einsum('qae,qpe->pae', remote, flux_other[side_index], precision=highest)
        result = result + jnp.einsum('ab,pae->pbe', projection[side_index], numeric, precision=highest)
    return result


def uplift_trace(trace_flat, seafloor_face):
    is_live = seafloor_face >= 0
    face_index = jnp.maximum(seafloor_face, 0)
    vertical = trace_flat[8 * NF:9 * NF]
    picked = jnp.take(vertical, face_index, axis=1)
    return jnp.where(is_live[None, :], picked, 0.0)


def pressure_term(load_trace, seafloor_face, projection, element_count):
    is_live = seafloor_face >= 0
    face_index = jnp.maximum(seafloor_face, 0)
    side_of_face = face_index // element_count
    element_index = face_index % element_count
    weighted = jnp.where(is_live[None, :], load_trace, 0.0)
    lifted = jnp.zeros((NB, seafloor_face.shape[0]), jnp.float32)
    for side_index in range(4):
        chosen = jnp.where(side_of_face[None, :] == side_index, weighted, 0.0)
        lifted = lifted + jnp.dot(projection[side_index].T, chosen, precision=highest)
    return jnp.zeros((NB, element_count), jnp.float32).at[:, element_index].add(lifted)


def element_update(state_local, jacobian_local, stiffness, projection, self_local, other_local,
                   source_local, mask_local, floor_local, integral, trace_flat, received, load_trace):
    neighbour_table = jnp.concatenate([trace_flat, received], axis=1)
    volume = volume_term(integral, jacobian_local, stiffness)
    flux_sum = flux_term(trace_flat, neighbour_table, source_local, self_local, other_local, projection)
    pressure = pressure_term(load_trace, floor_local, projection, state_local.shape[2])
    updated = state_local + volume - flux_sum
    updated = updated.at[2].add(-pressure)
    return jnp.where(mask_local[None, None, :] > 0, updated, state_local)


def split_devices(whole_array, partitions):
    shaped = whole_array.reshape(whole_array.shape[:-1] + (partitions, whole_array.shape[-1] // partitions))
    return jnp.moveaxis(shaped, -2, 0)


def from_below(arranged, position):
    length = arranged.shape[position]
    kept_part = lax.slice_in_dim(arranged, 0, length - 1, axis=position)
    zeros_rim = jnp.zeros_like(lax.slice_in_dim(arranged, 0, 1, axis=position))
    return jnp.concatenate([zeros_rim, kept_part], axis=position)


def from_above(arranged, position):
    length = arranged.shape[position]
    kept_part = lax.slice_in_dim(arranged, 1, length, axis=position)
    zeros_rim = jnp.zeros_like(lax.slice_in_dim(arranged, 0, 1, axis=position))
    return jnp.concatenate([kept_part, zeros_rim], axis=position)


def ocean_update(height, east_flow, north_flow, water_depth, source):
    padded_east = jnp.pad(east_flow, 1)
    padded_north = jnp.pad(north_flow, 1)
    east_slope = (padded_east[2:, 1:-1] - padded_east[:-2, 1:-1]) * 0.5
    north_slope = (padded_north[1:-1, 2:] - padded_north[1:-1, :-2]) * 0.5
    height_next = height + ocean_step * (source - water_depth * (east_slope + north_slope))
    padded_height = jnp.pad(height_next, 1)
    east_next = east_flow - ocean_step * (padded_height[2:, 1:-1] - padded_height[:-2, 1:-1]) * 0.5
    north_next = north_flow - ocean_step * (padded_height[1:-1, 2:] - padded_height[1:-1, :-2]) * 0.5
    return height_next, east_next, north_next


def reference(element_state, jacobians, stiffness, projection, flux_self, flux_other, face_source,
              send_faces, cluster_mask, seafloor_face, ocean_cell, ocean_weight, height, east_flow,
              north_flow, water_depth):
    partitions = N_GX * N_GY * N_GZ
    state_dev = split_devices(element_state, partitions)
    jacobian_dev = split_devices(jacobians, partitions)
    send_dev = split_devices(send_faces, partitions)
    floor_dev = split_devices(seafloor_face, partitions)

    def first_section(inputs):
        state_local, jacobian_local, send_local, floor_local = inputs
        integral = predictor(state_local, jacobian_local, stiffness)
        trace_flat = trace_table(integral, projection)
        outgoing = jnp.stack([jnp.take(trace_flat, send_local[direction], axis=1) for direction in range(6)])
        return integral, outgoing, uplift_trace(trace_flat, floor_local)

    integral_dev, outgoing_dev, uplift_dev = lax.map(first_section, (state_dev, jacobian_dev, send_dev, floor_dev))

    arranged = outgoing_dev.reshape((N_GX, N_GY, N_GZ, 6) + outgoing_dev.shape[2:])
    received = jnp.stack([
        from_below(arranged[:, :, :, 1], 0), from_above(arranged[:, :, :, 0], 0),
        from_below(arranged[:, :, :, 3], 1), from_above(arranged[:, :, :, 2], 1),
        from_below(arranged[:, :, :, 5], 2), from_above(arranged[:, :, :, 4], 2)], axis=3)
    received = received.reshape((partitions, 6) + received.shape[4:])
    received = jnp.moveaxis(received, 1, 2).reshape(partitions, NQ * NF, -1)

    tile_count = N_GX * N_GY
    slots_all = tile_count * SLOTS

    def to_tiles(field_grid):
        return field_grid.reshape(N_GX, CXO, N_GY, CYO).transpose(0, 2, 1, 3).reshape(tile_count, CXO * CYO)

    def from_tiles(tiled_grid):
        return tiled_grid.reshape(N_GX, N_GY, CXO, CYO).transpose(0, 2, 1, 3).reshape(N_GX * CXO, N_GY * CYO)

    uplift_grid = uplift_dev.reshape(tile_count, N_GZ, NF, tile_count, SLOTS).transpose(3, 1, 2, 0, 4)
    uplift_grid = uplift_grid.reshape(tile_count, N_GZ, NF, slots_all)
    uplift_values = jnp.sum(ocean_weight * uplift_grid, axis=2).reshape(tile_count, N_GZ * slots_all)
    cells_flat = ocean_cell.reshape(tile_count, N_GZ * slots_all)

    def scatter_tile(cells_tile, values_tile):
        return jnp.zeros((CXO * CYO,), jnp.float32).at[cells_tile].add(values_tile)

    source = from_tiles(jax.vmap(scatter_tile)(cells_flat, uplift_values))

    def pick_tile(heights_tile, cells_tile):
        return jnp.take(heights_tile, cells_tile)

    heights_at = jax.vmap(pick_tile)(to_tiles(height), ocean_cell)
    load_grid = ocean_weight * heights_at[:, :, None, :]
    load_dev = load_grid.reshape(tile_count, N_GZ, NF, tile_count, SLOTS).transpose(3, 1, 2, 0, 4)
    load_dev = load_dev.reshape(partitions, NF, slots_all)

    def second_section(inputs):
        (state_local, jacobian_local, self_local, other_local, source_local, mask_local,
         floor_local, integral, received_local, load_local) = inputs
        trace_flat = trace_table(integral, projection)
        return element_update(state_local, jacobian_local, stiffness, projection, self_local, other_local,
                              source_local, mask_local, floor_local, integral, trace_flat,
                              received_local, load_local)

    next_dev = lax.map(second_section, (
        state_dev, jacobian_dev, split_devices(flux_self, partitions), split_devices(flux_other, partitions),
        split_devices(face_source, partitions), split_devices(cluster_mask, partitions), floor_dev,
        integral_dev, received, load_dev))
    next_state = jnp.moveaxis(next_dev, 0, -2).reshape(NQ, NB, -1)
    new_height, new_east, new_north = ocean_update(height, east_flow, north_flow, water_depth, source)
    return (next_state, new_height, new_east, new_north)
```

```python
import jax
import jax.numpy as jnp
from jax import lax
from jax.experimental import pallas as pl
from jax.experimental.pallas import tpu as pltpu
from jax.sharding import PartitionSpec as P

NQ = 9
NB = 35
NF = 15
LN = 128
EL = NQ * LN
TILE = 256
SLAB = 1024
EDGE = EL + TILE

time_step = 1.5
ocean_step = 0.5
f32 = jnp.float32
bf16 = jnp.bfloat16
NT = (((1,), (1,)), ((), ()))


def cost(us):
    return pl.CostEstimate(flops=int(us * 2e8), bytes_accessed=1 << 20, transcendentals=0)


def shaped(*dims):
    return jax.ShapeDtypeStruct(dims, f32)


def split(x):
    high = x.astype(bf16)
    return high, (x - high.astype(f32)).astype(bf16)


def dot3(left, right):
    rows = left.shape[0]
    left_high, left_low = split(left)
    right_high, right_low = split(right)
    both = jnp.dot(
        jnp.concatenate([left_high, left_low], axis=0), right_high, preferred_element_type=f32
    )
    return both[:rows] + both[rows:] + jnp.dot(left_high, right_low, preferred_element_type=f32)


def block(q):
    return pl.ds(q * LN, LN)


def one_hot(row, count, value):
    lanes = row.shape[1]
    target = jnp.broadcast_to(row.astype(f32), (16, lanes)).astype(bf16)
    ids = lax.broadcasted_iota(jnp.int32, (16, lanes), 0).astype(f32)
    zero = jnp.zeros((16, lanes), bf16)
    hits = [target == (ids + 16.0 * c).astype(bf16) for c in range(count // 16)]
    return [jnp.concatenate([jnp.where(h, v, zero) for h in hits], axis=0) for v in value]


def pick(table, index, which, sources):
    found = jnp.zeros(index.shape, f32)
    for s in range(sources):
        taken = jnp.take_along_axis(table(s), index, axis=1)
        found = jnp.where(which == s, taken, found)
    return found


def as_row(column):
    size = column.shape[0]
    eye = lax.broadcasted_iota(jnp.int32, (size, size), 0) == lax.broadcasted_iota(
        jnp.int32, (size, size), 1
    )
    return jnp.sum(jnp.where(eye, column, 0.0), axis=0, keepdims=True)


def as_column(row):
    size = row.shape[1]
    eye = lax.broadcasted_iota(jnp.int32, (size, size), 0) == lax.broadcasted_iota(
        jnp.int32, (size, size), 1
    )
    return jnp.sum(jnp.where(eye, row, 0.0), axis=1, keepdims=True)


def neighbours(x, low_row, high_row):
    size = x.shape[0]
    ids = lax.broadcasted_iota(jnp.int32, x.shape, 0)
    after = jnp.where(ids == size - 1, high_row, pltpu.roll(x, size - 1, 0))
    before = jnp.where(ids == 0, low_row, pltpu.roll(x, 1, 0))
    return after - before


def neighbours_lanes(x, low_col, high_col):
    size = x.shape[1]
    ids = lax.broadcasted_iota(jnp.int32, x.shape, 1)
    after = jnp.where(ids == size - 1, high_col, pltpu.roll(x, size - 1, 1))
    before = jnp.where(ids == 0, low_col, pltpu.roll(x, 1, 1))
    return after - before


def lookup_kernel(meta, weight, cell, height, out, high_low):
    @pl.when(pl.program_id(0) == 0)
    def _():
        high, low = split(height[...])
        high_low[0:TILE] = high
        high_low[TILE:] = low

    layer = meta[0]
    base = pl.program_id(0) * SLAB
    one = jnp.ones((16, TILE), bf16)
    ids = lax.broadcasted_iota(jnp.int32, (TILE, TILE), 0)
    for pair in range(SLAB // TILE):
        start = pl.multiple_of(base + pair * TILE, TILE)
        cells = cell[0, 0:1, pl.ds(start, TILE)]
        for n in range(1, cell.shape[1]):
            cells = jnp.where(layer == n, cell[0, n : n + 1, pl.ds(start, TILE)], cells)
        rows, cols = (cells >> 8, cells & 255)
        (hot,) = one_hot(cols, TILE, [one])
        both = jnp.dot(high_low[...], hot, preferred_element_type=f32)
        found = both[:TILE] + both[TILE:]
        values = jnp.sum(jnp.where(ids == rows, found, 0.0), axis=0, keepdims=True)
        for half in range(2):
            t = 2 * pair + half
            out[t, 0:NF, :] = weight[0, 0, :, t * LN : (t + 1) * LN]
            out[t, NF : NF + 1, :] = values[:, half * LN : (half + 1) * LN]


def lookup(meta, ocean_weight, ocean_cell, height):
    steps = ocean_cell.shape[2] // SLAB
    per = SLAB // LN
    return pl.pallas_call(
        lookup_kernel,
        out_shape=shaped(steps * per, NF + 1, LN),
        grid_spec=pltpu.PrefetchScalarGridSpec(
            num_scalar_prefetch=1,
            grid=(steps,),
            in_specs=[
                pl.BlockSpec((1, 1, NF, SLAB), lambda s, m: (0, m[0], 0, s)),
                pl.BlockSpec(ocean_cell.shape, lambda s, m: (0, 0, 0)),
                pl.BlockSpec(height.shape, lambda s, m: (0, 0)),
            ],
            out_specs=pl.BlockSpec((per, NF + 1, LN), lambda s, m: (s, 0, 0)),
            scratch_shapes=[pltpu.VMEM((2 * TILE, TILE), bf16)],
        ),
        cost_estimate=cost(4),
        name="lookup",
    )(meta, ocean_weight, ocean_cell, height)


def spread_jacobians(jacobians, spread):
    for d in range(3):
        for p in range(NQ):
            for q in range(NQ):
                at = ((d * NQ + p) * NQ + q) * 8
                spread[at : at + 8] = jnp.broadcast_to(jacobians[d, p, q : q + 1, :], (8, LN))


def couple(spread, dof, coupled):
    def rows(b, carry):
        here = pl.ds(pl.multiple_of(b * 8, 8), 8)
        parts = [dof[here, q * LN : (q + 1) * LN] for q in range(NQ)]
        for d in range(3):
            for p in range(NQ):
                total = None
                for q in range(NQ):
                    at = ((d * NQ + p) * NQ + q) * 8
                    term = spread[at : at + 8] * parts[q]
                    total = term if total is None else total + term
                coupled[pl.ds(pl.multiple_of(d * 40 + b * 8, 8), 8), p * LN : (p + 1) * LN] = total
        return carry

    lax.fori_loop(0, 5, rows, 0)


def stiffness_rows(stiffness, pad, transposed):
    total = None
    for d in range(3):
        pad[...] = jnp.zeros((LN, LN), f32)
        pad[0:NB, 0:NB] = stiffness[d]
        value = pad[...].T[0:40] if transposed else pad[0:40]
        value = pltpu.roll(value, d * 40, 1) if d else value
        total = value if total is None else total + value
    return total


def face_rows(projection, pad):
    pad[...] = jnp.zeros((LN, LN), f32)
    for f in range(4):
        pad[f * 16 : f * 16 + NF, 0:NB] = projection[f]
    return pad


def predict_kernel(
    state, jacobians, stiffness, projection, send, east, north, integral, trace, sent,
    spread, dof, coupled, pad, index,
):
    spread_jacobians(jacobians, spread)
    coupled[...] = jnp.zeros((LN, EL), f32)
    dof[...] = jnp.zeros((40, EL), f32)
    for q in range(NQ):
        dof[0:NB, q * LN : (q + 1) * LN] = state[q]
    integral[...] = time_step * dof[...]
    matrix = stiffness_rows(stiffness, pad, False)

    def degree(n, weight):
        couple(spread, dof, coupled)
        current = -dot3(matrix, coupled[...])
        dof[...] = current
        weight = weight * time_step / (n + 2).astype(f32)
        integral[...] = integral[...] + weight * current
        return weight

    lax.fori_loop(0, 4, degree, jnp.float32(time_step))
    faces = face_rows(projection, pad)
    trace[...] = dot3(faces[0:64, 0:40], integral[...])
    index[...] = jnp.zeros((8, LN), jnp.int32)
    index[0:6, 0:16] = send[...]
    lane = lax.broadcasted_iota(jnp.int32, (8, LN), 1)
    wanted = jnp.zeros((8, LN), jnp.int32)
    for spot, direction in enumerate((1, 0, 3, 2, 5, 4)):
        row = jnp.broadcast_to(index[direction : direction + 1, :], (8, LN))
        row = pltpu.roll(row, 16 * spot, 1) if spot else row
        wanted = jnp.where(lane // 16 == spot, row, wanted)
    wanted = jnp.concatenate([wanted, wanted], axis=0)
    for q in range(NQ):
        sent[:, q * LN : (q + 1) * LN] = pick(
            lambda s: trace[s * 16 : (s + 1) * 16, q * LN : (q + 1) * LN],
            wanted & 127, wanted >> 7, 4,
        )
    sent[:, EL:] = jnp.zeros((16, TILE), f32)
    sent[0:1, EL:] = east[0:1, :]
    sent[1:2, EL:] = east[TILE - 1 : TILE, :]
    sent[2:3, EL:] = as_row(north[:, 0:1])
    sent[3:4, EL:] = as_row(north[:, TILE - 1 : TILE])


def predict(state, jacobians, stiffness, projection, send, east, north):
    return pl.pallas_call(
        predict_kernel,
        out_shape=(shaped(40, EL), shaped(64, EL), shaped(16, EDGE)),
        scratch_shapes=[
            pltpu.VMEM((243 * 8, LN), f32),
            pltpu.VMEM((40, EL), f32),
            pltpu.VMEM((LN, EL), f32),
            pltpu.VMEM((LN, LN), f32),
            pltpu.VMEM((8, LN), jnp.int32),
        ],
        cost_estimate=cost(10),
        name="predict",
    )(state, jacobians, stiffness, projection, send, east, north)


def uplift_kernel(inbound, trace, floor, out):
    def tile(r, carry):
        face = jnp.broadcast_to(floor[pl.ds(r, 1), :], (16, LN))
        found = pick(
            lambda s: trace[s * 16 : (s + 1) * 16, 8 * LN : 9 * LN], face & 127, face >> 7, 4
        )
        out[pl.ds(r, 1), :] = jnp.sum(inbound[r] * found, axis=0, keepdims=True)
        return carry

    lax.fori_loop(0, floor.shape[0], tile, 0, unroll=8)


def uplift(inbound, trace, floor):
    return pl.pallas_call(
        uplift_kernel, out_shape=shaped(*floor.shape), cost_estimate=cost(2), name="uplift"
    )(inbound, trace, floor)


def volume_kernel(
    state, jacobians, stiffness, integral, inbound, floor, base, load, spread, coupled, pad, left, right
):
    spread_jacobians(jacobians, spread)
    coupled[...] = jnp.zeros((LN, EL), f32)
    couple(spread, integral, coupled)
    volume = dot3(stiffness_rows(stiffness, pad, True), coupled[...])
    base[...] = volume
    for q in range(NQ):
        here = pl.ds(q * LN, LN)
        base[0:NB, here] = volume[0:NB, q * LN : (q + 1) * LN] + state[q]
    zero = jnp.zeros((16, LN), bf16)
    one = jnp.ones((16, LN), bf16)

    def chunk(c, total):
        for i in range(8):
            r = c * 8 + i
            lanes = slice(i * LN, (i + 1) * LN)
            face = floor[pl.ds(r, 1), :]
            part = inbound[r]
            high, low = split(part * part[NF : NF + 1, :])
            (hot,) = one_hot(face & 127, LN, [one])
            right[:, lanes] = hot
            side = jnp.broadcast_to((face >> 7).astype(f32), (16, LN)).astype(bf16)
            for f in range(4):
                hit = side == jnp.full((16, LN), f, bf16)
                left[f * 16 : (f + 1) * 16, lanes] = jnp.where(hit, high, zero)
                left[64 + f * 16 : 64 + (f + 1) * 16, lanes] = jnp.where(hit, low, zero)
        return total + lax.dot_general(left[...], right[...], NT, preferred_element_type=f32)

    total = lax.fori_loop(0, floor.shape[0] // 8, chunk, jnp.zeros((LN, LN), f32))
    load[...] = total[:64] + total[64:]


def volume(state, jacobians, stiffness, integral, inbound, floor):
    return pl.pallas_call(
        volume_kernel,
        out_shape=(shaped(40, EL), shaped(64, LN)),
        scratch_shapes=[
            pltpu.VMEM((243 * 8, LN), f32),
            pltpu.VMEM((LN, EL), f32),
            pltpu.VMEM((LN, LN), f32),
            pltpu.VMEM((LN, SLAB), bf16),
            pltpu.VMEM((LN, SLAB), bf16),
        ],
        cost_estimate=cost(6),
        name="volume",
    )(state, jacobians, stiffness, integral, inbound, floor)


def flux_kernel(
    meta, state, base, load, trace, below_x, above_x, below_y, above_y, below_z, above_z,
    source, own, other, projection, mask, out, numeric, received, pad,
):
    faces = face_rows(projection, pad)
    matrix = faces[...].T[0:40, 0:64]
    lane = lax.broadcasted_iota(jnp.int32, (16, LN), 1)
    sides = (
        (below_x, meta[1] > 0), (above_x, meta[1] < meta[4] - 1),
        (below_y, meta[2] > 0), (above_y, meta[2] < meta[5] - 1),
        (below_z, meta[0] > 0), (above_z, meta[0] < meta[3] - 1),
    )
    low = [jnp.where(there, 16 * n, LN) for n, (_, there) in enumerate(sides)]
    for q in range(NQ):
        here = slice(q * LN, (q + 1) * LN)
        found = jnp.zeros((16, LN), f32)
        for n, (side, _) in enumerate(sides):
            hit = (lane >= low[n]) & (lane < low[n] + 16)
            found = jnp.where(hit, side[:, here], found)
        received[:, here] = found

    def face(f, carry):
        which = jnp.broadcast_to(source[pl.ds(f, 1), :], (16, LN))
        rows = pl.ds(pl.multiple_of(f * 16, 16), 16)
        total = [None] * NQ
        for q in range(NQ):
            here = slice(q * LN, (q + 1) * LN)
            mine = trace[rows, here]
            remote = pick(
                lambda s: received[:, here] if s == 4 else trace[s * 16 : (s + 1) * 16, here],
                which & 127, which >> 7, 5,
            )
            for p in range(NQ):
                term = mine * own[f, q, p : p + 1, :] + remote * other[f, q, p : p + 1, :]
                total[p] = term if total[p] is None else total[p] + term
        for p in range(NQ):
            numeric[rows, p * LN : (p + 1) * LN] = total[p]
        return carry

    lax.fori_loop(0, 4, face, 0)
    numeric[:, 2 * LN : 3 * LN] = numeric[:, 2 * LN : 3 * LN] + load[...]
    taken = dot3(matrix, numeric[...])
    updated = base[...] - taken
    live = mask[...] > 0
    for p in range(NQ):
        out[p] = jnp.where(live, updated[0:NB, p * LN : (p + 1) * LN], state[p])


def flux(meta, state, base, load, trace, received, source, own, other, projection, mask):
    smem = pl.BlockSpec(memory_space=pltpu.SMEM)
    vmem = pl.BlockSpec(memory_space=pltpu.VMEM)
    return pl.pallas_call(
        flux_kernel,
        out_shape=shaped(NQ, NB, LN),
        in_specs=[smem] + [vmem] * 15,
        out_specs=vmem,
        scratch_shapes=[
            pltpu.VMEM((64, EL), f32),
            pltpu.VMEM((16, EL), f32),
            pltpu.VMEM((LN, LN), f32),
        ],
        cost_estimate=cost(6),
        name="flux",
    )(meta, state, base, load, trace, *received, source, own, other, projection, mask)


def ocean_kernel(
    meta, first, second, third, fourth, cell, below_x, above_x, below_y, above_y,
    height, east, north, depth, new_height, edges, left, right, total, lifts,
):
    layers = meta[3]
    per = first.shape[0]
    total[...] = jnp.zeros((2 * TILE, TILE), f32)
    one = jnp.ones((16, LN), bf16)
    for shift, values in enumerate((first, second, third, fourth)):
        layer = lax.rem(meta[0] - shift + layers, layers)
        lifts[pl.ds(pl.multiple_of(layer * per, 8), per)] = values[...]
    for layer in range(4):

        def chunk(c, carry):
            for i in range(8):
                r = c * 8 + i
                lanes = slice(i * LN, (i + 1) * LN)
                start = pl.multiple_of(r * LN, LN)
                cells = cell[0, layer : layer + 1, pl.ds(start, LN)]
                value = jnp.broadcast_to(lifts[pl.ds(layer * per + r, 1), :], (16, LN))
                high, low = one_hot(cells >> 8, TILE, split(value))
                left[0:TILE, lanes] = high
                left[TILE:, lanes] = low
                (right[:, lanes],) = one_hot(cells & 255, TILE, [one])
            total[...] += lax.dot_general(
                left[...], right[...], NT, preferred_element_type=f32
            )
            return carry

        lax.fori_loop(0, per // 8, chunk, 0)
    source = total[0:TILE] + total[TILE:]
    rim = slice(EL, EDGE)
    low_x = jnp.where(meta[1] > 0, below_x[1:2, rim], 0.0)
    high_x = jnp.where(meta[1] < meta[4] - 1, above_x[0:1, rim], 0.0)
    low_y = as_column(jnp.where(meta[2] > 0, below_y[3:4, rim], 0.0))
    high_y = as_column(jnp.where(meta[2] < meta[5] - 1, above_y[2:3, rim], 0.0))
    slope = neighbours(east[...], low_x, high_x) * 0.5
    slope = slope + neighbours_lanes(north[...], low_y, high_y) * 0.5
    updated = height[...] + ocean_step * (source - depth[...] * slope)
    new_height[...] = updated
    edges[...] = jnp.zeros((8, TILE), f32)
    edges[0:1] = updated[0:1, :]
    edges[1:2] = updated[TILE - 1 : TILE, :]
    edges[2:3] = as_row(updated[:, 0:1])
    edges[3:4] = as_row(updated[:, TILE - 1 : TILE])


def ocean(meta, layers, cell, received, height, east, north, depth):
    smem = pl.BlockSpec(memory_space=pltpu.SMEM)
    vmem = pl.BlockSpec(memory_space=pltpu.VMEM)
    return pl.pallas_call(
        ocean_kernel,
        out_shape=(shaped(TILE, TILE), shaped(8, TILE)),
        in_specs=[smem] + [vmem] * 13,
        out_specs=(vmem, vmem),
        scratch_shapes=[
            pltpu.VMEM((2 * TILE, SLAB), bf16),
            pltpu.VMEM((TILE, SLAB), bf16),
            pltpu.VMEM((2 * TILE, TILE), f32),
            pltpu.VMEM((4 * layers[0].shape[0], LN), f32),
        ],
        cost_estimate=cost(10),
        name="ocean",
    )(meta, *layers, cell, *received[:4], height, east, north, depth)


def flow_kernel(meta, height, east, north, below_x, above_x, below_y, above_y, new_east, new_north):
    low_x = jnp.where(meta[1] > 0, below_x[1:2], 0.0)
    high_x = jnp.where(meta[1] < meta[4] - 1, above_x[0:1], 0.0)
    low_y = as_column(jnp.where(meta[2] > 0, below_y[3:4], 0.0))
    high_y = as_column(jnp.where(meta[2] < meta[5] - 1, above_y[2:3], 0.0))
    level = height[...]
    new_east[...] = east[...] - ocean_step * neighbours(level, low_x, high_x) * 0.5
    new_north[...] = north[...] - ocean_step * neighbours_lanes(level, low_y, high_y) * 0.5


def flow(meta, height, east, north, received):
    smem = pl.BlockSpec(memory_space=pltpu.SMEM)
    vmem = pl.BlockSpec(memory_space=pltpu.VMEM)
    return pl.pallas_call(
        flow_kernel,
        out_shape=(shaped(TILE, TILE), shaped(TILE, TILE)),
        in_specs=[smem] + [vmem] * 7,
        out_specs=(vmem, vmem),
        cost_estimate=cost(2),
        name="flow",
    )(meta, height, east, north, *received)


def shifted(value, axis, step):
    count = lax.axis_size(axis)
    return lax.ppermute(value, axis, [(i, (i + step) % count) for i in range(count)])


def on_device(
    element_state,
    jacobians,
    stiffness,
    projection,
    flux_self,
    flux_other,
    face_source,
    send_faces,
    cluster_mask,
    seafloor_face,
    ocean_cell,
    ocean_weight,
    height,
    east_flow,
    north_flow,
    water_depth,
):
    names = ("gz", "gx", "gy")
    spot = jnp.arange(8, dtype=jnp.int32)
    meta = jnp.zeros((8,), jnp.int32)
    for n, axis in enumerate(names):
        meta = jnp.where(spot == n, lax.axis_index(axis).astype(jnp.int32), meta)
        meta = jnp.where(spot == n + 3, lax.axis_size(axis), meta)
    floor = seafloor_face.reshape(-1, LN)
    mask = cluster_mask.reshape(1, LN)
    outbound = lookup(meta, ocean_weight, ocean_cell, height)
    inbound = lax.all_to_all(outbound, ("gx", "gy"), 0, 0, tiled=True)
    integral, trace, sent = predict(
        element_state, jacobians, stiffness, projection, send_faces, east_flow, north_flow
    )
    lifted = uplift(inbound, trace, floor)
    landed = lax.all_to_all(lifted, ("gx", "gy"), 0, 0, tiled=True)
    received = [shifted(sent, axis, step) for axis in ("gx", "gy", "gz") for step in (1, -1)]
    layers = [landed] + [shifted(landed, "gz", step) for step in (1, 2, 3)]
    base, load = volume(element_state, jacobians, stiffness, integral, inbound, floor)
    new_height, edges = ocean(
        meta, layers, ocean_cell, received, height, east_flow, north_flow, water_depth
    )
    rims = [shifted(edges, axis, step) for axis in ("gx", "gy") for step in (1, -1)]
    next_state = flux(
        meta, element_state, base, load, trace, received, face_source, flux_self, flux_other,
        projection, mask,
    )
    new_east, new_north = flow(meta, new_height, east_flow, north_flow, rims)
    return (next_state, new_height, new_east, new_north)


def solution(mesh):
    return jax.shard_map(
        on_device,
        mesh=mesh,
        in_specs=(
            P(None, None, ("gx", "gy", "gz")),
            P(None, None, None, ("gx", "gy", "gz")),
            P(),
            P(),
            P(None, None, None, ("gx", "gy", "gz")),
            P(None, None, None, ("gx", "gy", "gz")),
            P(None, ("gx", "gy", "gz")),
            P(None, ("gx", "gy", "gz")),
            P(("gx", "gy", "gz")),
            P(("gx", "gy", "gz")),
            P(("gx", "gy"), None, None),
            P(("gx", "gy"), None, None, None),
            P("gx", "gy"),
            P("gx", "gy"),
            P("gx", "gy"),
            P("gx", "gy"),
        ),
        out_specs=(P(None, None, ("gx", "gy", "gz")), P("gx", "gy"), P("gx", "gy"), P("gx", "gy")),
        check_vma=False,
    )
```

```python
import jax
import jax.numpy as jnp
from jax import lax
from jax.experimental import pallas as pl
from jax.experimental.pallas import tpu as pltpu
from jax.sharding import PartitionSpec as P

NQ = 9
NB = 35
NF = 15
LN = 128
EL = NQ * LN
TILE = 256
SLAB = 1024
EDGE = EL + TILE

time_step = 1.5
ocean_step = 0.5
f32 = jnp.float32
bf16 = jnp.bfloat16
NT = (((1,), (1,)), ((), ()))


def cost(us):
    return pl.CostEstimate(flops=int(us * 2e8), bytes_accessed=1 << 20, transcendentals=0)


def limit(mib):
    return pltpu.CompilerParams(vmem_limit_bytes=mib << 20)


def shaped(*dims):
    return jax.ShapeDtypeStruct(dims, f32)


def split(x):
    high = x.astype(bf16)
    return high, (x - high.astype(f32)).astype(bf16)


def dot3(left, right):
    rows = left.shape[0]
    left_high, left_low = split(left)
    right_high, right_low = split(right)
    both = jnp.dot(
        jnp.concatenate([left_high, left_low], axis=0), right_high, preferred_element_type=f32
    )
    return both[:rows] + both[rows:] + jnp.dot(left_high, right_low, preferred_element_type=f32)


def block(q):
    return pl.ds(q * LN, LN)


def one_hot(row, count, value):
    lanes = row.shape[1]
    target = jnp.broadcast_to(row.astype(f32), (16, lanes)).astype(bf16)
    ids = lax.broadcasted_iota(jnp.int32, (16, lanes), 0).astype(f32)
    zero = jnp.zeros((16, lanes), bf16)
    hits = [target == (ids + 16.0 * c).astype(bf16) for c in range(count // 16)]
    return [jnp.concatenate([jnp.where(h, v, zero) for h in hits], axis=0) for v in value]


def joined(left, right):
    whole = [jnp.concatenate([r[i] for i in range(8)], axis=1) for r in (left, right)]
    return lax.dot_general(*whole, NT, preferred_element_type=f32)


def pick(table, index, which, sources):
    found = jnp.zeros(index.shape, f32)
    for s in range(sources):
        taken = jnp.take_along_axis(table(s), index, axis=1)
        found = jnp.where(which == s, taken, found)
    return found


def as_row(column):
    size = column.shape[0]
    eye = lax.broadcasted_iota(jnp.int32, (size, size), 0) == lax.broadcasted_iota(
        jnp.int32, (size, size), 1
    )
    return jnp.sum(jnp.where(eye, column, 0.0), axis=0, keepdims=True)


def as_column(row):
    size = row.shape[1]
    eye = lax.broadcasted_iota(jnp.int32, (size, size), 0) == lax.broadcasted_iota(
        jnp.int32, (size, size), 1
    )
    return jnp.sum(jnp.where(eye, row, 0.0), axis=1, keepdims=True)


def neighbours(x, low_row, high_row):
    size = x.shape[0]
    ids = lax.broadcasted_iota(jnp.int32, x.shape, 0)
    after = jnp.where(ids == size - 1, high_row, pltpu.roll(x, size - 1, 0))
    before = jnp.where(ids == 0, low_row, pltpu.roll(x, 1, 0))
    return after - before


def neighbours_lanes(x, low_col, high_col):
    size = x.shape[1]
    ids = lax.broadcasted_iota(jnp.int32, x.shape, 1)
    after = jnp.where(ids == size - 1, high_col, pltpu.roll(x, size - 1, 1))
    before = jnp.where(ids == 0, low_col, pltpu.roll(x, 1, 1))
    return after - before


def arrange_kernel(weight, out):
    for t in range(SLAB // LN):
        out[t, 0:NF, :] = weight[:, t * LN : (t + 1) * LN]
        out[t, NF : NF + 1, :] = jnp.zeros((1, LN), f32)


def arrange(weight):
    steps = weight.shape[1] // SLAB
    per = SLAB // LN
    return pl.pallas_call(
        arrange_kernel,
        out_shape=shaped(steps * per, NF + 1, LN),
        grid=(steps,),
        in_specs=[pl.BlockSpec((NF, SLAB), lambda s: (0, s))],
        out_specs=pl.BlockSpec((per, NF + 1, LN), lambda s: (s, 0, 0)),
        compiler_params=limit(8),
        cost_estimate=cost(1),
        name="arrange",
    )(weight)


def lookup_kernel(meta, cell, height, out, high_low):
    high, low = split(height[...])
    high_low[0:TILE] = high
    high_low[TILE:] = low
    layer = meta[0]
    one = jnp.ones((16, TILE), bf16)
    ids = lax.broadcasted_iota(jnp.int32, (TILE, TILE), 0)

    def pair(c, carry):
        for half in range(4):
            t = c * 8 + half * 2
            start = pl.multiple_of(t * LN, TILE)
            cells = cell[0, 0:1, pl.ds(start, TILE)]
            for n in range(1, cell.shape[1]):
                cells = jnp.where(layer == n, cell[0, n : n + 1, pl.ds(start, TILE)], cells)
            rows, cols = (cells >> 8, cells & 255)
            (hot,) = one_hot(cols, TILE, [one])
            both = jnp.dot(high_low[...], hot, preferred_element_type=f32)
            found = both[:TILE] + both[TILE:]
            values = jnp.sum(jnp.where(ids == rows, found, 0.0), axis=0, keepdims=True)
            out[pl.ds(t, 1), :] = values[:, 0:LN]
            out[pl.ds(t + 1, 1), :] = values[:, LN:]
        return carry

    lax.fori_loop(0, out.shape[0] // 8, pair, 0)


def lookup(meta, ocean_cell, height):
    smem = pl.BlockSpec(memory_space=pltpu.SMEM)
    vmem = pl.BlockSpec(memory_space=pltpu.VMEM)
    return pl.pallas_call(
        lookup_kernel,
        out_shape=shaped(ocean_cell.shape[2] // LN, LN),
        in_specs=[smem, vmem, vmem],
        out_specs=vmem,
        scratch_shapes=[pltpu.VMEM((2 * TILE, TILE), bf16)],
        compiler_params=limit(16),
        cost_estimate=cost(6),
        name="lookup",
    )(meta, ocean_cell, height)


def spread_jacobians(jacobians, spread):
    for d in range(3):
        for p in range(NQ):
            for q in range(NQ):
                at = ((d * NQ + p) * NQ + q) * 8
                spread[at : at + 8] = jnp.broadcast_to(jacobians[p, q, d : d + 1, :], (8, LN))


def couple(spread, dof, coupled):
    def rows(b, carry):
        here = pl.ds(pl.multiple_of(b * 8, 8), 8)
        parts = [dof[here, q * LN : (q + 1) * LN] for q in range(NQ)]
        for d in range(3):
            for p in range(NQ):
                total = None
                for q in range(NQ):
                    at = ((d * NQ + p) * NQ + q) * 8
                    term = spread[at : at + 8] * parts[q]
                    total = term if total is None else total + term
                coupled[pl.ds(pl.multiple_of(d * 40 + b * 8, 8), 8), p * LN : (p + 1) * LN] = total
        return carry

    lax.fori_loop(0, 5, rows, 0)


def stiffness_rows(stiffness, pad, transposed):
    total = None
    for d in range(3):
        pad[...] = jnp.zeros((LN, LN), f32)
        pad[0:NB, 0:NB] = stiffness[d]
        value = pad[...].T[0:40] if transposed else pad[0:40]
        value = pltpu.roll(value, d * 40, 1) if d else value
        total = value if total is None else total + value
    return total


def face_rows(projection, pad):
    pad[...] = jnp.zeros((LN, LN), f32)
    for f in range(4):
        for a in range(NF):
            pad[f * 16 + a : f * 16 + a + 1, 0:NB] = projection[a, f : f + 1, :]
    return pad


def predict_kernel(
    state, jacobians, stiffness, projection, send, east, north, integral, trace, sent,
    spread, dof, coupled, pad, index,
):
    spread_jacobians(jacobians, spread)
    coupled[...] = jnp.zeros((LN, EL), f32)
    dof[...] = jnp.zeros((40, EL), f32)
    for q in range(NQ):
        dof[0:NB, q * LN : (q + 1) * LN] = state[q]
    integral[...] = time_step * dof[...]
    matrix = stiffness_rows(stiffness, pad, False)

    def degree(n, weight):
        couple(spread, dof, coupled)
        current = -dot3(matrix, coupled[...])
        dof[...] = current
        weight = weight * time_step / (n + 2).astype(f32)
        integral[...] = integral[...] + weight * current
        return weight

    lax.fori_loop(0, 4, degree, jnp.float32(time_step))
    faces = face_rows(projection, pad)
    trace[...] = dot3(faces[0:64, 0:40], integral[...])
    index[...] = jnp.zeros((8, LN), jnp.int32)
    index[0:6, 0:16] = send[...]
    lane = lax.broadcasted_iota(jnp.int32, (8, LN), 1)
    wanted = jnp.zeros((8, LN), jnp.int32)
    for spot, direction in enumerate((1, 0, 3, 2, 5, 4)):
        row = jnp.broadcast_to(index[direction : direction + 1, :], (8, LN))
        row = pltpu.roll(row, 16 * spot, 1) if spot else row
        wanted = jnp.where(lane // 16 == spot, row, wanted)
    wanted = jnp.concatenate([wanted, wanted], axis=0)
    for q in range(NQ):
        sent[:, q * LN : (q + 1) * LN] = pick(
            lambda s: trace[s * 16 : (s + 1) * 16, q * LN : (q + 1) * LN],
            wanted & 127, wanted >> 7, 4,
        )
    sent[:, EL:] = jnp.zeros((16, TILE), f32)
    sent[0:1, EL:] = east[0:1, :]
    sent[1:2, EL:] = east[TILE - 1 : TILE, :]
    sent[2:3, EL:] = as_row(north[:, 0:1])
    sent[3:4, EL:] = as_row(north[:, TILE - 1 : TILE])


def predict(state, jacobians, stiffness, projection, send, east, north):
    return pl.pallas_call(
        predict_kernel,
        out_shape=(shaped(40, EL), shaped(64, EL), shaped(16, EDGE)),
        scratch_shapes=[
            pltpu.VMEM((243 * 8, LN), f32),
            pltpu.VMEM((40, EL), f32),
            pltpu.VMEM((LN, EL), f32),
            pltpu.VMEM((LN, LN), f32),
            pltpu.VMEM((8, LN), jnp.int32),
        ],
        compiler_params=limit(24),
        cost_estimate=cost(5),
        name="predict",
    )(state, jacobians, stiffness, projection, send, east, north)


def uplift_kernel(inbound, trace, floor, heights, out):
    def tile(r, carry):
        face = jnp.broadcast_to(floor[pl.ds(r, 1), :], (16, LN))
        found = pick(
            lambda s: trace[s * 16 : (s + 1) * 16, 8 * LN : 9 * LN], face & 127, face >> 7, 4
        )
        out[r, 0:1, :] = jnp.sum(inbound[r] * found, axis=0, keepdims=True)
        out[r, 1:2, :] = heights[pl.ds(r, 1), :]
        return carry

    lax.fori_loop(0, floor.shape[0], tile, 0, unroll=8)


def uplift(inbound, trace, floor, heights):
    return pl.pallas_call(
        uplift_kernel,
        out_shape=shaped(floor.shape[0], 2, LN),
        compiler_params=limit(16),
        cost_estimate=cost(2),
        name="uplift",
    )(inbound, trace, floor, heights)


def volume_kernel(state, jacobians, stiffness, integral, base, spread, coupled, pad):
    spread_jacobians(jacobians, spread)
    coupled[...] = jnp.zeros((LN, EL), f32)
    couple(spread, integral, coupled)
    volume = dot3(stiffness_rows(stiffness, pad, True), coupled[...])
    base[...] = volume
    for q in range(NQ):
        base[0:NB, q * LN : (q + 1) * LN] = volume[0:NB, q * LN : (q + 1) * LN] + state[q]


def volume(state, jacobians, stiffness, integral):
    return pl.pallas_call(
        volume_kernel,
        out_shape=shaped(40, EL),
        scratch_shapes=[
            pltpu.VMEM((243 * 8, LN), f32),
            pltpu.VMEM((LN, EL), f32),
            pltpu.VMEM((LN, LN), f32),
        ],
        compiler_params=limit(16),
        cost_estimate=cost(3),
        name="volume",
    )(state, jacobians, stiffness, integral)


def pressure_kernel(inbound, landed, floor, load, left, right):
    zero = jnp.zeros((16, LN), bf16)
    one = jnp.ones((16, LN), bf16)

    def chunk(c, total):
        for i in range(8):
            r = c * 8 + i
            face = floor[pl.ds(r, 1), :]
            high, low = split(inbound[r] * landed[r, 1:2, :])
            (right[i],) = one_hot(face & 127, LN, [one])
            side = jnp.broadcast_to((face >> 7).astype(f32), (16, LN)).astype(bf16)
            for f in range(4):
                hit = side == jnp.full((16, LN), f, bf16)
                left[i, f * 16 : (f + 1) * 16] = jnp.where(hit, high, zero)
                left[i, 64 + f * 16 : 64 + (f + 1) * 16] = jnp.where(hit, low, zero)
        return total + joined(left, right)

    total = lax.fori_loop(0, floor.shape[0] // 8, chunk, jnp.zeros((LN, LN), f32))
    load[...] = total[:64] + total[64:]


def pressure(inbound, landed, floor):
    return pl.pallas_call(
        pressure_kernel,
        out_shape=shaped(64, LN),
        scratch_shapes=[pltpu.VMEM((8, LN, LN), bf16), pltpu.VMEM((8, LN, LN), bf16)],
        compiler_params=limit(16),
        cost_estimate=cost(3),
        name="pressure",
    )(inbound, landed, floor)


def flux_kernel(
    meta, state, base, load, trace, below_x, above_x, below_y, above_y, below_z, above_z,
    source, own, other, projection, mask, out, numeric, received, pad,
):
    faces = face_rows(projection, pad)
    matrix = faces[...].T[0:40, 0:64]
    lane = lax.broadcasted_iota(jnp.int32, (16, LN), 1)
    sides = (
        (below_x, meta[1] > 0), (above_x, meta[1] < meta[4] - 1),
        (below_y, meta[2] > 0), (above_y, meta[2] < meta[5] - 1),
        (below_z, meta[0] > 0), (above_z, meta[0] < meta[3] - 1),
    )
    low = [jnp.where(there, 16 * n, LN) for n, (_, there) in enumerate(sides)]
    for q in range(NQ):
        here = slice(q * LN, (q + 1) * LN)
        found = jnp.zeros((16, LN), f32)
        for n, (side, _) in enumerate(sides):
            hit = (lane >= low[n]) & (lane < low[n] + 16)
            found = jnp.where(hit, side[:, here], found)
        received[:, here] = found

    for f in range(4):
        which = jnp.broadcast_to(source[f : f + 1, :], (16, LN))
        rows = slice(f * 16, (f + 1) * 16)
        total = [None] * NQ
        for q in range(NQ):
            here = slice(q * LN, (q + 1) * LN)
            mine = trace[rows, here]
            remote = pick(
                lambda s: received[:, here] if s == 4 else trace[s * 16 : (s + 1) * 16, here],
                which & 127, which >> 7, 5,
            )
            for p in range(NQ):
                term = mine * own[q, p, f : f + 1, :] + remote * other[q, p, f : f + 1, :]
                total[p] = term if total[p] is None else total[p] + term
        for p in range(NQ):
            numeric[rows, p * LN : (p + 1) * LN] = total[p]
    numeric[:, 2 * LN : 3 * LN] = numeric[:, 2 * LN : 3 * LN] + load[...]
    taken = dot3(matrix, numeric[...])
    updated = base[...] - taken
    live = mask[...] > 0
    for p in range(NQ):
        out[p] = jnp.where(live, updated[0:NB, p * LN : (p + 1) * LN], state[p])


def flux(meta, state, base, load, trace, received, source, own, other, projection, mask):
    smem = pl.BlockSpec(memory_space=pltpu.SMEM)
    vmem = pl.BlockSpec(memory_space=pltpu.VMEM)
    return pl.pallas_call(
        flux_kernel,
        out_shape=shaped(NQ, NB, LN),
        in_specs=[smem] + [vmem] * 15,
        out_specs=vmem,
        scratch_shapes=[
            pltpu.VMEM((64, EL), f32),
            pltpu.VMEM((16, EL), f32),
            pltpu.VMEM((LN, LN), f32),
        ],
        compiler_params=limit(16),
        cost_estimate=cost(4),
        name="flux",
    )(meta, state, base, load, trace, *received, source, own, other, projection, mask)


def ocean_kernel(
    meta, first, second, third, fourth, cell, below_x, above_x, below_y, above_y,
    height, east, north, depth, new_height, edges,
    left_a, right_a, left_b, right_b, total, lifts,
):
    layers = meta[3]
    per = first.shape[0]
    total[...] = jnp.zeros((2 * TILE, TILE), f32)
    one = jnp.ones((16, LN), bf16)
    for shift, values in enumerate((first, second, third, fourth)):
        layer = lax.rem(meta[0] - shift + layers, layers)
        lifts[pl.ds(pl.multiple_of(layer * per, 8), per)] = values[:, 0, :]

    def build(c, left, right):
        for half in range(2):
            t = c * 2 + half
            cells = cell[0, :, pl.ds(pl.multiple_of(t * LN, LN), LN)]
            for layer in range(4):
                here = cells[layer : layer + 1, :]
                value = jnp.broadcast_to(lifts[pl.ds(layer * per + t, 1), :], (16, LN))
                high, low = one_hot(here >> 8, TILE, split(value))
                left[half * 4 + layer, 0:TILE] = high
                left[half * 4 + layer, TILE:] = low
                (right[half * 4 + layer],) = one_hot(here & 255, TILE, [one])

    def chunks(c, carry):
        build(2 * c + 1, left_b, right_b)
        total[...] += joined(left_a, right_a)
        build(jnp.minimum(2 * c + 2, per // 2 - 1), left_a, right_a)
        total[...] += joined(left_b, right_b)
        return carry

    build(0, left_a, right_a)
    lax.fori_loop(0, per // 4, chunks, 0)
    source = total[0:TILE] + total[TILE:]
    rim = slice(EL, EDGE)
    low_x = jnp.where(meta[1] > 0, below_x[1:2, rim], 0.0)
    high_x = jnp.where(meta[1] < meta[4] - 1, above_x[0:1, rim], 0.0)
    low_y = as_column(jnp.where(meta[2] > 0, below_y[3:4, rim], 0.0))
    high_y = as_column(jnp.where(meta[2] < meta[5] - 1, above_y[2:3, rim], 0.0))
    slope = neighbours(east[...], low_x, high_x) * 0.5
    slope = slope + neighbours_lanes(north[...], low_y, high_y) * 0.5
    updated = height[...] + ocean_step * (source - depth[...] * slope)
    new_height[...] = updated
    edges[...] = jnp.zeros((8, TILE), f32)
    edges[0:1] = updated[0:1, :]
    edges[1:2] = updated[TILE - 1 : TILE, :]
    edges[2:3] = as_row(updated[:, 0:1])
    edges[3:4] = as_row(updated[:, TILE - 1 : TILE])


def ocean(meta, layers, cell, received, height, east, north, depth):
    smem = pl.BlockSpec(memory_space=pltpu.SMEM)
    vmem = pl.BlockSpec(memory_space=pltpu.VMEM)
    return pl.pallas_call(
        ocean_kernel,
        out_shape=(shaped(TILE, TILE), shaped(8, TILE)),
        in_specs=[smem] + [vmem] * 13,
        out_specs=(vmem, vmem),
        scratch_shapes=[
            pltpu.VMEM((8, 2 * TILE, LN), bf16),
            pltpu.VMEM((8, TILE, LN), bf16),
            pltpu.VMEM((8, 2 * TILE, LN), bf16),
            pltpu.VMEM((8, TILE, LN), bf16),
            pltpu.VMEM((2 * TILE, TILE), f32),
            pltpu.VMEM((4 * layers[0].shape[0], LN), f32),
        ],
        compiler_params=limit(32),
        cost_estimate=cost(10),
        name="ocean",
    )(meta, *layers, cell, *received[:4], height, east, north, depth)


def flow_kernel(meta, height, east, north, below_x, above_x, below_y, above_y, new_east, new_north):
    low_x = jnp.where(meta[1] > 0, below_x[1:2], 0.0)
    high_x = jnp.where(meta[1] < meta[4] - 1, above_x[0:1], 0.0)
    low_y = as_column(jnp.where(meta[2] > 0, below_y[3:4], 0.0))
    high_y = as_column(jnp.where(meta[2] < meta[5] - 1, above_y[2:3], 0.0))
    level = height[...]
    new_east[...] = east[...] - ocean_step * neighbours(level, low_x, high_x) * 0.5
    new_north[...] = north[...] - ocean_step * neighbours_lanes(level, low_y, high_y) * 0.5


def flow(meta, height, east, north, received):
    smem = pl.BlockSpec(memory_space=pltpu.SMEM)
    vmem = pl.BlockSpec(memory_space=pltpu.VMEM)
    return pl.pallas_call(
        flow_kernel,
        out_shape=(shaped(TILE, TILE), shaped(TILE, TILE)),
        in_specs=[smem] + [vmem] * 7,
        out_specs=(vmem, vmem),
        compiler_params=limit(16),
        cost_estimate=cost(2),
        name="flow",
    )(meta, height, east, north, *received)


def shifted(value, axis, step):
    count = lax.axis_size(axis)
    return lax.ppermute(value, axis, [(i, (i + step) % count) for i in range(count)])


def on_device(
    element_state,
    jacobians,
    stiffness,
    projection,
    flux_self,
    flux_other,
    face_source,
    send_faces,
    cluster_mask,
    seafloor_face,
    ocean_cell,
    ocean_weight,
    height,
    east_flow,
    north_flow,
    water_depth,
):
    names = ("gz", "gx", "gy")
    spot = jnp.arange(8, dtype=jnp.int32)
    meta = jnp.zeros((8,), jnp.int32)
    for n, axis in enumerate(names):
        meta = jnp.where(spot == n, lax.axis_index(axis).astype(jnp.int32), meta)
        meta = jnp.where(spot == n + 3, lax.axis_size(axis), meta)
    floor = seafloor_face.reshape(-1, LN)
    mask = cluster_mask.reshape(1, LN)
    jacobians, flux_self, flux_other = (
        jnp.transpose(x, (1, 2, 0, 3)) for x in (jacobians, flux_self, flux_other)
    )
    projection = jnp.transpose(projection, (1, 0, 2))
    weight = lax.dynamic_index_in_dim(ocean_weight[0], lax.axis_index("gz"), 0, keepdims=False)
    inbound = lax.all_to_all(arrange(weight), ("gx", "gy"), 0, 0, tiled=True)
    integral, trace, sent = predict(
        element_state, jacobians, stiffness, projection, send_faces, east_flow, north_flow
    )
    heights = lookup(meta, ocean_cell, height)
    lifted = uplift(inbound, trace, floor, heights)
    landed = lax.all_to_all(lifted, ("gx", "gy"), 0, 0, tiled=True)
    received = [shifted(sent, axis, step) for axis in ("gx", "gy", "gz") for step in (1, -1)]
    layers = [landed] + [shifted(landed, "gz", step) for step in (1, 2, 3)]
    base = volume(element_state, jacobians, stiffness, integral)
    load = pressure(inbound, landed, floor)
    new_height, edges = ocean(
        meta, layers, ocean_cell, received, height, east_flow, north_flow, water_depth
    )
    rims = [shifted(edges, axis, step) for axis in ("gx", "gy") for step in (1, -1)]
    next_state = flux(
        meta, element_state, base, load, trace, received, face_source, flux_self, flux_other,
        projection, mask,
    )
    new_east, new_north = flow(meta, new_height, east_flow, north_flow, rims)
    return (next_state, new_height, new_east, new_north)


def solution(mesh):
    return jax.shard_map(
        on_device,
        mesh=mesh,
        in_specs=(
            P(None, None, ("gx", "gy", "gz")),
            P(None, None, None, ("gx", "gy", "gz")),
            P(),
            P(),
            P(None, None, None, ("gx", "gy", "gz")),
            P(None, None, None, ("gx", "gy", "gz")),
            P(None, ("gx", "gy", "gz")),
            P(None, ("gx", "gy", "gz")),
            P(("gx", "gy", "gz")),
            P(("gx", "gy", "gz")),
            P(("gx", "gy"), None, None),
            P(("gx", "gy"), None, None, None),
            P("gx", "gy"),
            P("gx", "gy"),
            P("gx", "gy"),
            P("gx", "gy"),
        ),
        out_specs=(P(None, None, ("gx", "gy", "gz")), P("gx", "gy"), P("gx", "gy"), P("gx", "gy")),
        check_vma=False,
    )
```

```python
import jax
import jax.numpy as jnp
from jax import lax
from jax.experimental import pallas as pl
from jax.experimental.pallas import tpu as pltpu
from jax.sharding import PartitionSpec as P

NQ = 9
NB = 35
NF = 15
LN = 128
EL = NQ * LN
TILE = 256
SLAB = 1024
EDGE = EL + TILE

time_step = 1.5
ocean_step = 0.5
f32 = jnp.float32
bf16 = jnp.bfloat16
NT = (((1,), (1,)), ((), ()))


def cost(us):
    return pl.CostEstimate(flops=int(us * 2e8), bytes_accessed=1 << 20, transcendentals=0)


def limit(mib):
    return pltpu.CompilerParams(vmem_limit_bytes=mib << 20)


def shaped(*dims):
    return jax.ShapeDtypeStruct(dims, f32)


def split(x):
    high = x.astype(bf16)
    return high, (x - high.astype(f32)).astype(bf16)


def dot3(left, right):
    rows = left.shape[0]
    left_high, left_low = split(left)
    right_high, right_low = split(right)
    both = jnp.dot(
        jnp.concatenate([left_high, left_low], axis=0), right_high, preferred_element_type=f32
    )
    return both[:rows] + both[rows:] + jnp.dot(left_high, right_low, preferred_element_type=f32)


def block(q):
    return pl.ds(q * LN, LN)


def one_hot(row, count, value):
    lanes = row.shape[1]
    target = jnp.broadcast_to(row.astype(f32), (16, lanes)).astype(bf16)
    ids = lax.broadcasted_iota(jnp.int32, (16, lanes), 0).astype(f32)
    zero = jnp.zeros((16, lanes), bf16)
    hits = [target == (ids + 16.0 * c).astype(bf16) for c in range(count // 16)]
    return [jnp.concatenate([jnp.where(h, v, zero) for h in hits], axis=0) for v in value]


def joined(left, right):
    whole = [jnp.concatenate([r[i] for i in range(8)], axis=1) for r in (left, right)]
    return lax.dot_general(*whole, NT, preferred_element_type=f32)


def pick(table, index, which, sources):
    found = jnp.zeros(index.shape, f32)
    for s in range(sources):
        taken = jnp.take_along_axis(table(s), index, axis=1)
        found = jnp.where(which == s, taken, found)
    return found


def as_row(column):
    size = column.shape[0]
    eye = lax.broadcasted_iota(jnp.int32, (size, size), 0) == lax.broadcasted_iota(
        jnp.int32, (size, size), 1
    )
    return jnp.sum(jnp.where(eye, column, 0.0), axis=0, keepdims=True)


def as_column(row):
    size = row.shape[1]
    eye = lax.broadcasted_iota(jnp.int32, (size, size), 0) == lax.broadcasted_iota(
        jnp.int32, (size, size), 1
    )
    return jnp.sum(jnp.where(eye, row, 0.0), axis=1, keepdims=True)


def neighbours(x, low_row, high_row):
    size = x.shape[0]
    ids = lax.broadcasted_iota(jnp.int32, x.shape, 0)
    after = jnp.where(ids == size - 1, high_row, pltpu.roll(x, size - 1, 0))
    before = jnp.where(ids == 0, low_row, pltpu.roll(x, 1, 0))
    return after - before


def neighbours_lanes(x, low_col, high_col):
    size = x.shape[1]
    ids = lax.broadcasted_iota(jnp.int32, x.shape, 1)
    after = jnp.where(ids == size - 1, high_col, pltpu.roll(x, size - 1, 1))
    before = jnp.where(ids == 0, low_col, pltpu.roll(x, 1, 1))
    return after - before


def arrange_kernel(meta, weight, out):
    for n in range(weight.shape[2]):

        @pl.when(meta[0] == n)
        def _():
            for t in range(SLAB // LN):
                for a in range(NF):
                    out[t, a : a + 1, :] = weight[0, a, n : n + 1, t * LN : (t + 1) * LN]

    out[:, NF : NF + 1, :] = jnp.zeros((SLAB // LN, 1, LN), f32)


def arrange(meta, weight):
    steps = weight.shape[3] // SLAB
    per = SLAB // LN
    return pl.pallas_call(
        arrange_kernel,
        out_shape=shaped(steps * per, NF + 1, LN),
        grid=(steps,),
        in_specs=[
            pl.BlockSpec(memory_space=pltpu.SMEM),
            pl.BlockSpec((1, NF, weight.shape[2], SLAB), lambda s: (0, 0, 0, s)),
        ],
        out_specs=pl.BlockSpec((per, NF + 1, LN), lambda s: (s, 0, 0)),
        compiler_params=limit(8),
        cost_estimate=cost(1),
        name="arrange",
    )(meta, weight)


def lookup_kernel(meta, cell, height, out, high_low):
    high, low = split(height[...])
    high_low[0:TILE] = high
    high_low[TILE:] = low
    layer = meta[0]
    one = jnp.ones((16, TILE), bf16)
    ids = lax.broadcasted_iota(jnp.int32, (TILE, TILE), 0)

    def pair(c, carry):
        for half in range(4):
            t = c * 8 + half * 2
            start = pl.multiple_of(t * LN, TILE)
            cells = cell[0, 0:1, pl.ds(start, TILE)]
            for n in range(1, cell.shape[1]):
                cells = jnp.where(layer == n, cell[0, n : n + 1, pl.ds(start, TILE)], cells)
            rows, cols = (cells >> 8, cells & 255)
            (hot,) = one_hot(cols, TILE, [one])
            both = jnp.dot(high_low[...], hot, preferred_element_type=f32)
            found = both[:TILE] + both[TILE:]
            values = jnp.sum(jnp.where(ids == rows, found, 0.0), axis=0, keepdims=True)
            out[pl.ds(t, 1), :] = values[:, 0:LN]
            out[pl.ds(t + 1, 1), :] = values[:, LN:]
        return carry

    lax.fori_loop(0, out.shape[0] // 8, pair, 0)


def lookup(meta, ocean_cell, height):
    smem = pl.BlockSpec(memory_space=pltpu.SMEM)
    vmem = pl.BlockSpec(memory_space=pltpu.VMEM)
    return pl.pallas_call(
        lookup_kernel,
        out_shape=shaped(ocean_cell.shape[2] // LN, LN),
        in_specs=[smem, vmem, vmem],
        out_specs=vmem,
        scratch_shapes=[pltpu.VMEM((2 * TILE, TILE), bf16)],
        compiler_params=limit(16),
        cost_estimate=cost(6),
        name="lookup",
    )(meta, ocean_cell, height)


def spread_jacobians(jacobians, spread):
    for d in range(3):
        for p in range(NQ):
            for q in range(NQ):
                at = ((d * NQ + p) * NQ + q) * 8
                spread[at : at + 8] = jnp.broadcast_to(jacobians[p, q, d : d + 1, :], (8, LN))


def couple(spread, dof, coupled):
    def rows(b, carry):
        here = pl.ds(pl.multiple_of(b * 8, 8), 8)
        parts = [dof[here, q * LN : (q + 1) * LN] for q in range(NQ)]
        for d in range(3):
            for p in range(NQ):
                total = None
                for q in range(NQ):
                    at = ((d * NQ + p) * NQ + q) * 8
                    term = spread[at : at + 8] * parts[q]
                    total = term if total is None else total + term
                coupled[pl.ds(pl.multiple_of(d * 40 + b * 8, 8), 8), p * LN : (p + 1) * LN] = total
        return carry

    lax.fori_loop(0, 5, rows, 0)


def stiffness_rows(stiffness, pad, transposed):
    total = None
    for d in range(3):
        pad[...] = jnp.zeros((LN, LN), f32)
        pad[0:NB, 0:NB] = stiffness[d]
        value = pad[...].T[0:40] if transposed else pad[0:40]
        value = pltpu.roll(value, d * 40, 1) if d else value
        total = value if total is None else total + value
    return total


def face_rows(projection, pad):
    pad[...] = jnp.zeros((LN, LN), f32)
    for f in range(4):
        for a in range(NF):
            pad[f * 16 + a : f * 16 + a + 1, 0:NB] = projection[a, f : f + 1, :]
    return pad


def predict_kernel(
    state, jacobians, stiffness, projection, send, east, north, base, trace, sent,
    spread, dof, coupled, pad, index, integral,
):
    spread_jacobians(jacobians, spread)
    coupled[...] = jnp.zeros((LN, EL), f32)
    dof[...] = jnp.zeros((40, EL), f32)
    for q in range(NQ):
        dof[0:NB, q * LN : (q + 1) * LN] = state[q]
    integral[...] = time_step * dof[...]
    matrix = stiffness_rows(stiffness, pad, False)

    def degree(n, weight):
        couple(spread, dof, coupled)
        current = -dot3(matrix, coupled[...])
        dof[...] = current
        weight = weight * time_step / (n + 2).astype(f32)
        integral[...] = integral[...] + weight * current
        return weight

    lax.fori_loop(0, 4, degree, jnp.float32(time_step))
    faces = face_rows(projection, pad)
    trace[...] = dot3(faces[0:64, 0:40], integral[...])
    index[...] = jnp.zeros((8, LN), jnp.int32)
    index[0:6, 0:16] = send[...]
    lane = lax.broadcasted_iota(jnp.int32, (8, LN), 1)
    wanted = jnp.zeros((8, LN), jnp.int32)
    for spot, direction in enumerate((1, 0, 3, 2, 5, 4)):
        row = jnp.broadcast_to(index[direction : direction + 1, :], (8, LN))
        row = pltpu.roll(row, 16 * spot, 1) if spot else row
        wanted = jnp.where(lane // 16 == spot, row, wanted)
    wanted = jnp.concatenate([wanted, wanted], axis=0)
    for q in range(NQ):
        sent[:, q * LN : (q + 1) * LN] = pick(
            lambda s: trace[s * 16 : (s + 1) * 16, q * LN : (q + 1) * LN],
            wanted & 127, wanted >> 7, 4,
        )
    sent[:, EL:] = jnp.zeros((16, TILE), f32)
    sent[0:1, EL:] = east[0:1, :]
    sent[1:2, EL:] = east[TILE - 1 : TILE, :]
    sent[2:3, EL:] = as_row(north[:, 0:1])
    sent[3:4, EL:] = as_row(north[:, TILE - 1 : TILE])
    couple(spread, integral, coupled)
    volume = dot3(stiffness_rows(stiffness, pad, True), coupled[...])
    base[...] = volume
    for q in range(NQ):
        base[0:NB, q * LN : (q + 1) * LN] = volume[0:NB, q * LN : (q + 1) * LN] + state[q]


def predict(state, jacobians, stiffness, projection, send, east, north):
    return pl.pallas_call(
        predict_kernel,
        out_shape=(shaped(40, EL), shaped(64, EL), shaped(16, EDGE)),
        scratch_shapes=[
            pltpu.VMEM((243 * 8, LN), f32),
            pltpu.VMEM((40, EL), f32),
            pltpu.VMEM((LN, EL), f32),
            pltpu.VMEM((LN, LN), f32),
            pltpu.VMEM((8, LN), jnp.int32),
            pltpu.VMEM((40, EL), f32),
        ],
        compiler_params=limit(24),
        cost_estimate=cost(4),
        name="predict",
    )(state, jacobians, stiffness, projection, send, east, north)


def uplift_kernel(inbound, trace, floor, heights, out):
    def tile(r, carry):
        face = jnp.broadcast_to(floor[pl.ds(r, 1), :], (16, LN))
        found = pick(
            lambda s: trace[s * 16 : (s + 1) * 16, 8 * LN : 9 * LN], face & 127, face >> 7, 4
        )
        out[r, 0:1, :] = jnp.sum(inbound[r] * found, axis=0, keepdims=True)
        out[r, 1:2, :] = heights[pl.ds(r, 1), :]
        return carry

    lax.fori_loop(0, floor.shape[0], tile, 0, unroll=8)


def uplift(inbound, trace, floor, heights):
    return pl.pallas_call(
        uplift_kernel,
        out_shape=shaped(floor.shape[0], 2, LN),
        compiler_params=limit(16),
        cost_estimate=cost(2),
        name="uplift",
    )(inbound, trace, floor, heights)


def pressure_kernel(inbound, landed, floor, load, left, right):
    zero = jnp.zeros((16, LN), bf16)
    one = jnp.ones((16, LN), bf16)

    def chunk(c, total):
        for i in range(8):
            r = c * 8 + i
            face = floor[pl.ds(r, 1), :]
            high, low = split(inbound[r] * landed[r, 1:2, :])
            (right[i],) = one_hot(face & 127, LN, [one])
            side = jnp.broadcast_to((face >> 7).astype(f32), (16, LN)).astype(bf16)
            for f in range(4):
                hit = side == jnp.full((16, LN), f, bf16)
                left[i, f * 16 : (f + 1) * 16] = jnp.where(hit, high, zero)
                left[i, 64 + f * 16 : 64 + (f + 1) * 16] = jnp.where(hit, low, zero)
        return total + joined(left, right)

    total = lax.fori_loop(0, floor.shape[0] // 8, chunk, jnp.zeros((LN, LN), f32))
    load[...] = total[:64] + total[64:]


def pressure(inbound, landed, floor):
    return pl.pallas_call(
        pressure_kernel,
        out_shape=shaped(64, LN),
        scratch_shapes=[pltpu.VMEM((8, LN, LN), bf16), pltpu.VMEM((8, LN, LN), bf16)],
        compiler_params=limit(16),
        cost_estimate=cost(3),
        name="pressure",
    )(inbound, landed, floor)


def flux_kernel(
    meta, state, base, load, trace, below_x, above_x, below_y, above_y, below_z, above_z,
    source, own, other, projection, mask, out, numeric, received, pad,
):
    faces = face_rows(projection, pad)
    matrix = faces[...].T[0:40, 0:64]
    lane = lax.broadcasted_iota(jnp.int32, (16, LN), 1)
    sides = (
        (below_x, meta[1] > 0), (above_x, meta[1] < meta[4] - 1),
        (below_y, meta[2] > 0), (above_y, meta[2] < meta[5] - 1),
        (below_z, meta[0] > 0), (above_z, meta[0] < meta[3] - 1),
    )
    low = [jnp.where(there, 16 * n, LN) for n, (_, there) in enumerate(sides)]
    for q in range(NQ):
        here = slice(q * LN, (q + 1) * LN)
        found = jnp.zeros((16, LN), f32)
        for n, (side, _) in enumerate(sides):
            hit = (lane >= low[n]) & (lane < low[n] + 16)
            found = jnp.where(hit, side[:, here], found)
        received[:, here] = found

    for f in range(4):
        which = jnp.broadcast_to(source[f : f + 1, :], (16, LN))
        rows = slice(f * 16, (f + 1) * 16)
        total = [None] * NQ
        for q in range(NQ):
            here = slice(q * LN, (q + 1) * LN)
            mine = trace[rows, here]
            remote = pick(
                lambda s: received[:, here] if s == 4 else trace[s * 16 : (s + 1) * 16, here],
                which & 127, which >> 7, 5,
            )
            for p in range(NQ):
                term = mine * own[q, p, f : f + 1, :] + remote * other[q, p, f : f + 1, :]
                total[p] = term if total[p] is None else total[p] + term
        for p in range(NQ):
            numeric[rows, p * LN : (p + 1) * LN] = total[p]
    numeric[:, 2 * LN : 3 * LN] = numeric[:, 2 * LN : 3 * LN] + load[...]
    taken = dot3(matrix, numeric[...])
    updated = base[...] - taken
    live = mask[...] > 0
    for p in range(NQ):
        out[p] = jnp.where(live, updated[0:NB, p * LN : (p + 1) * LN], state[p])


def flux(meta, state, base, load, trace, received, source, own, other, projection, mask):
    smem = pl.BlockSpec(memory_space=pltpu.SMEM)
    vmem = pl.BlockSpec(memory_space=pltpu.VMEM)
    return pl.pallas_call(
        flux_kernel,
        out_shape=shaped(NQ, NB, LN),
        in_specs=[smem] + [vmem] * 15,
        out_specs=vmem,
        scratch_shapes=[
            pltpu.VMEM((64, EL), f32),
            pltpu.VMEM((16, EL), f32),
            pltpu.VMEM((LN, LN), f32),
        ],
        compiler_params=limit(16),
        cost_estimate=cost(4),
        name="flux",
    )(meta, state, base, load, trace, *received, source, own, other, projection, mask)


def ocean_kernel(
    meta, first, second, third, fourth, cell, below_x, above_x, below_y, above_y,
    height, east, north, depth, new_height, edges, total, lifts,
):
    layers = meta[3]
    per = first.shape[0]
    total[...] = jnp.zeros((2 * TILE, TILE), f32)
    one = jnp.ones((16, LN), bf16)
    for shift, values in enumerate((first, second, third, fourth)):
        layer = lax.rem(meta[0] - shift + layers, layers)
        lifts[pl.ds(pl.multiple_of(layer * per, 8), per)] = values[:, 0, :]

    def chunk(c, carry):
        for half in range(2):
            t = c * 2 + half
            cells = cell[0, :, pl.ds(pl.multiple_of(t * LN, LN), LN)]
            for pair in range(2):
                left, right = [], []
                for layer in (2 * pair, 2 * pair + 1):
                    here = cells[layer : layer + 1, :]
                    value = jnp.broadcast_to(lifts[pl.ds(layer * per + t, 1), :], (16, LN))
                    left.append(jnp.concatenate(one_hot(here >> 8, TILE, split(value)), axis=0))
                    right += one_hot(here & 255, TILE, [one])
                total[...] += lax.dot_general(
                    jnp.concatenate(left, axis=1), jnp.concatenate(right, axis=1), NT,
                    preferred_element_type=f32,
                )
        return carry

    lax.fori_loop(0, per // 2, chunk, 0, unroll=8)
    source = total[0:TILE] + total[TILE:]
    rim = slice(EL, EDGE)
    low_x = jnp.where(meta[1] > 0, below_x[1:2, rim], 0.0)
    high_x = jnp.where(meta[1] < meta[4] - 1, above_x[0:1, rim], 0.0)
    low_y = as_column(jnp.where(meta[2] > 0, below_y[3:4, rim], 0.0))
    high_y = as_column(jnp.where(meta[2] < meta[5] - 1, above_y[2:3, rim], 0.0))
    slope = neighbours(east[...], low_x, high_x) * 0.5
    slope = slope + neighbours_lanes(north[...], low_y, high_y) * 0.5
    updated = height[...] + ocean_step * (source - depth[...] * slope)
    new_height[...] = updated
    edges[...] = jnp.zeros((8, TILE), f32)
    edges[0:1] = updated[0:1, :]
    edges[1:2] = updated[TILE - 1 : TILE, :]
    edges[2:3] = as_row(updated[:, 0:1])
    edges[3:4] = as_row(updated[:, TILE - 1 : TILE])


def ocean(meta, layers, cell, received, height, east, north, depth):
    smem = pl.BlockSpec(memory_space=pltpu.SMEM)
    vmem = pl.BlockSpec(memory_space=pltpu.VMEM)
    return pl.pallas_call(
        ocean_kernel,
        out_shape=(shaped(TILE, TILE), shaped(8, TILE)),
        in_specs=[smem] + [vmem] * 13,
        out_specs=(vmem, vmem),
        scratch_shapes=[
            pltpu.VMEM((2 * TILE, TILE), f32),
            pltpu.VMEM((4 * layers[0].shape[0], LN), f32),
        ],
        compiler_params=limit(32),
        cost_estimate=cost(10),
        name="ocean",
    )(meta, *layers, cell, *received[:4], height, east, north, depth)


def flow_kernel(meta, height, east, north, below_x, above_x, below_y, above_y, new_east, new_north):
    low_x = jnp.where(meta[1] > 0, below_x[1:2], 0.0)
    high_x = jnp.where(meta[1] < meta[4] - 1, above_x[0:1], 0.0)
    low_y = as_column(jnp.where(meta[2] > 0, below_y[3:4], 0.0))
    high_y = as_column(jnp.where(meta[2] < meta[5] - 1, above_y[2:3], 0.0))
    level = height[...]
    new_east[...] = east[...] - ocean_step * neighbours(level, low_x, high_x) * 0.5
    new_north[...] = north[...] - ocean_step * neighbours_lanes(level, low_y, high_y) * 0.5


def flow(meta, height, east, north, received):
    smem = pl.BlockSpec(memory_space=pltpu.SMEM)
    vmem = pl.BlockSpec(memory_space=pltpu.VMEM)
    return pl.pallas_call(
        flow_kernel,
        out_shape=(shaped(TILE, TILE), shaped(TILE, TILE)),
        in_specs=[smem] + [vmem] * 7,
        out_specs=(vmem, vmem),
        compiler_params=limit(16),
        cost_estimate=cost(2),
        name="flow",
    )(meta, height, east, north, *received)


def shifted(value, axis, step):
    count = lax.axis_size(axis)
    return lax.ppermute(value, axis, [(i, (i + step) % count) for i in range(count)])


def on_device(
    element_state,
    jacobians,
    stiffness,
    projection,
    flux_self,
    flux_other,
    face_source,
    send_faces,
    cluster_mask,
    seafloor_face,
    ocean_cell,
    ocean_weight,
    height,
    east_flow,
    north_flow,
    water_depth,
):
    names = ("gz", "gx", "gy")
    spot = jnp.arange(8, dtype=jnp.int32)
    meta = jnp.zeros((8,), jnp.int32)
    for n, axis in enumerate(names):
        meta = jnp.where(spot == n, lax.axis_index(axis).astype(jnp.int32), meta)
        meta = jnp.where(spot == n + 3, lax.axis_size(axis), meta)
    floor = seafloor_face.reshape(-1, LN)
    mask = cluster_mask.reshape(1, LN)
    jacobians, flux_self, flux_other = (
        jnp.transpose(x, (1, 2, 0, 3)) for x in (jacobians, flux_self, flux_other)
    )
    projection = jnp.transpose(projection, (1, 0, 2))
    weight = jnp.transpose(ocean_weight, (0, 2, 1, 3))
    inbound = lax.all_to_all(arrange(meta, weight), ("gx", "gy"), 0, 0, tiled=True)
    base, trace, sent = predict(
        element_state, jacobians, stiffness, projection, send_faces, east_flow, north_flow
    )
    heights = lookup(meta, ocean_cell, height)
    early = [shifted(sent, "gz", step) for step in (1, -1)]
    inbound, *early = lax.optimization_barrier((inbound, *early))
    lifted = uplift(inbound, trace, floor, heights)
    landed = lax.all_to_all(lifted, ("gx", "gy"), 0, 0, tiled=True)
    received = [shifted(sent, axis, step) for axis in ("gx", "gy") for step in (1, -1)] + early
    layers = [landed] + [shifted(landed, "gz", step) for step in (1, 2, 3)]
    load = pressure(inbound, landed, floor)
    new_height, edges = ocean(
        meta, layers, ocean_cell, received, height, east_flow, north_flow, water_depth
    )
    rims = [shifted(edges, axis, step) for axis in ("gx", "gy") for step in (1, -1)]
    next_state = flux(
        meta, element_state, base, load, trace, received, face_source, flux_self, flux_other,
        projection, mask,
    )
    new_east, new_north = flow(meta, new_height, east_flow, north_flow, rims)
    return (next_state, new_height, new_east, new_north)


def solution(mesh):
    return jax.shard_map(
        on_device,
        mesh=mesh,
        in_specs=(
            P(None, None, ("gx", "gy", "gz")),
            P(None, None, None, ("gx", "gy", "gz")),
            P(),
            P(),
            P(None, None, None, ("gx", "gy", "gz")),
            P(None, None, None, ("gx", "gy", "gz")),
            P(None, ("gx", "gy", "gz")),
            P(None, ("gx", "gy", "gz")),
            P(("gx", "gy", "gz")),
            P(("gx", "gy", "gz")),
            P(("gx", "gy"), None, None),
            P(("gx", "gy"), None, None, None),
            P("gx", "gy"),
            P("gx", "gy"),
            P("gx", "gy"),
            P("gx", "gy"),
        ),
        out_specs=(P(None, None, ("gx", "gy", "gz")), P("gx", "gy"), P("gx", "gy"), P("gx", "gy")),
        check_vma=False,
    )
```

```python
import jax
import jax.numpy as jnp
from jax import lax
from jax.experimental import pallas as pl
from jax.experimental.pallas import tpu as pltpu
from jax.sharding import PartitionSpec as P

NQ = 9
NB = 35
NF = 15
LN = 128
EL = NQ * LN
TILE = 256
SLAB = 1024
WIDE = 2048
EDGE = EL + TILE

time_step = 1.5
ocean_step = 0.5
f32 = jnp.float32
bf16 = jnp.bfloat16
NT = (((1,), (1,)), ((), ()))


def cost(us):
    return pl.CostEstimate(flops=int(us * 2e8), bytes_accessed=1 << 20, transcendentals=0)


def limit(mib):
    return pltpu.CompilerParams(vmem_limit_bytes=mib << 20)


def shaped(*dims):
    return jax.ShapeDtypeStruct(dims, f32)


def split(x):
    high = x.astype(bf16)
    return high, (x - high.astype(f32)).astype(bf16)


def dot3(left, right):
    rows = left.shape[0]
    left_high, left_low = split(left)
    right_high, right_low = split(right)
    both = jnp.dot(
        jnp.concatenate([left_high, left_low], axis=0), right_high, preferred_element_type=f32
    )
    return both[:rows] + both[rows:] + jnp.dot(left_high, right_low, preferred_element_type=f32)


def block(q):
    return pl.ds(q * LN, LN)


def one_hot(row, count, value):
    lanes = row.shape[1]
    target = jnp.broadcast_to(row.astype(f32), (16, lanes)).astype(bf16)
    ids = lax.broadcasted_iota(jnp.int32, (16, lanes), 0).astype(f32)
    zero = jnp.zeros((16, lanes), bf16)
    hits = [target == (ids + 16.0 * c).astype(bf16) for c in range(count // 16)]
    return [jnp.concatenate([jnp.where(h, v, zero) for h in hits], axis=0) for v in value]


def joined(left, right):
    whole = [jnp.concatenate([r[i] for i in range(8)], axis=1) for r in (left, right)]
    return lax.dot_general(*whole, NT, preferred_element_type=f32)


def pick(table, index, which, sources):
    found = jnp.zeros(index.shape, f32)
    for s in range(sources):
        taken = jnp.take_along_axis(table(s), index, axis=1)
        found = jnp.where(which == s, taken, found)
    return found


def as_row(column):
    size = column.shape[0]
    eye = lax.broadcasted_iota(jnp.int32, (size, size), 0) == lax.broadcasted_iota(
        jnp.int32, (size, size), 1
    )
    return jnp.sum(jnp.where(eye, column, 0.0), axis=0, keepdims=True)


def as_column(row):
    size = row.shape[1]
    eye = lax.broadcasted_iota(jnp.int32, (size, size), 0) == lax.broadcasted_iota(
        jnp.int32, (size, size), 1
    )
    return jnp.sum(jnp.where(eye, row, 0.0), axis=1, keepdims=True)


def neighbours(x, low_row, high_row):
    size = x.shape[0]
    ids = lax.broadcasted_iota(jnp.int32, x.shape, 0)
    after = jnp.where(ids == size - 1, high_row, pltpu.roll(x, size - 1, 0))
    before = jnp.where(ids == 0, low_row, pltpu.roll(x, 1, 0))
    return after - before


def neighbours_lanes(x, low_col, high_col):
    size = x.shape[1]
    ids = lax.broadcasted_iota(jnp.int32, x.shape, 1)
    after = jnp.where(ids == size - 1, high_col, pltpu.roll(x, size - 1, 1))
    before = jnp.where(ids == 0, low_col, pltpu.roll(x, 1, 1))
    return after - before


def arrange_kernel(meta, weight, out):
    for n in range(weight.shape[2]):

        @pl.when(meta[0] == n)
        def _():
            for t in range(WIDE // LN):
                for a in range(NF):
                    out[t, a : a + 1, :] = weight[0, a, n : n + 1, t * LN : (t + 1) * LN]

    out[:, NF : NF + 1, :] = jnp.zeros((WIDE // LN, 1, LN), f32)


def arrange(meta, weight):
    steps = weight.shape[3] // WIDE
    per = WIDE // LN
    return pl.pallas_call(
        arrange_kernel,
        out_shape=shaped(steps * per, NF + 1, LN),
        grid=(steps,),
        in_specs=[
            pl.BlockSpec(memory_space=pltpu.SMEM),
            pl.BlockSpec((1, NF, weight.shape[2], WIDE), lambda s: (0, 0, 0, s)),
        ],
        out_specs=pl.BlockSpec((per, NF + 1, LN), lambda s: (s, 0, 0)),
        compiler_params=limit(60),
        cost_estimate=cost(1),
        name="arrange",
    )(meta, weight)


def lookup_kernel(meta, cell, height, out, high_low):
    high, low = split(height[...])
    high_low[0:TILE] = high
    high_low[TILE:] = low
    layer = meta[0]
    one = jnp.ones((16, TILE), bf16)
    ids = lax.broadcasted_iota(jnp.int32, (TILE, TILE), 0)

    def pair(c, carry):
        for half in range(4):
            t = c * 8 + half * 2
            start = pl.multiple_of(t * LN, TILE)
            cells = cell[0, 0:1, pl.ds(start, TILE)]
            for n in range(1, cell.shape[1]):
                cells = jnp.where(layer == n, cell[0, n : n + 1, pl.ds(start, TILE)], cells)
            rows, cols = (cells >> 8, cells & 255)
            (hot,) = one_hot(cols, TILE, [one])
            both = jnp.dot(high_low[...], hot, preferred_element_type=f32)
            found = both[:TILE] + both[TILE:]
            values = jnp.sum(jnp.where(ids == rows, found, 0.0), axis=0, keepdims=True)
            out[pl.ds(t, 1), :] = values[:, 0:LN]
            out[pl.ds(t + 1, 1), :] = values[:, LN:]
        return carry

    lax.fori_loop(0, out.shape[0] // 8, pair, 0)


def lookup(meta, ocean_cell, height):
    smem = pl.BlockSpec(memory_space=pltpu.SMEM)
    vmem = pl.BlockSpec(memory_space=pltpu.VMEM)
    return pl.pallas_call(
        lookup_kernel,
        out_shape=shaped(ocean_cell.shape[2] // LN, LN),
        in_specs=[smem, vmem, vmem],
        out_specs=vmem,
        scratch_shapes=[pltpu.VMEM((2 * TILE, TILE), bf16)],
        compiler_params=limit(16),
        cost_estimate=cost(6),
        name="lookup",
    )(meta, ocean_cell, height)


def spread_jacobians(jacobians, spread):
    for d in range(3):
        for p in range(NQ):
            for q in range(NQ):
                at = ((d * NQ + p) * NQ + q) * 8
                spread[at : at + 8] = jnp.broadcast_to(jacobians[p, q, d : d + 1, :], (8, LN))


def couple(spread, dof, coupled):
    def rows(b, carry):
        here = pl.ds(pl.multiple_of(b * 8, 8), 8)
        parts = [dof[here, q * LN : (q + 1) * LN] for q in range(NQ)]
        for d in range(3):
            for p in range(NQ):
                total = None
                for q in range(NQ):
                    at = ((d * NQ + p) * NQ + q) * 8
                    term = spread[at : at + 8] * parts[q]
                    total = term if total is None else total + term
                coupled[pl.ds(pl.multiple_of(d * 40 + b * 8, 8), 8), p * LN : (p + 1) * LN] = total
        return carry

    lax.fori_loop(0, 5, rows, 0)


def stiffness_rows(stiffness, pad, transposed):
    total = None
    for d in range(3):
        pad[...] = jnp.zeros((LN, LN), f32)
        pad[0:NB, 0:NB] = stiffness[d]
        value = pad[...].T[0:40] if transposed else pad[0:40]
        value = pltpu.roll(value, d * 40, 1) if d else value
        total = value if total is None else total + value
    return total


def face_rows(projection, pad):
    pad[...] = jnp.zeros((LN, LN), f32)
    for f in range(4):
        for a in range(NF):
            pad[f * 16 + a : f * 16 + a + 1, 0:NB] = projection[a, f : f + 1, :]
    return pad


def predict_kernel(
    state, jacobians, stiffness, projection, send, east, north, base, trace, sent,
    spread, dof, coupled, pad, index, integral,
):
    spread_jacobians(jacobians, spread)
    coupled[...] = jnp.zeros((LN, EL), f32)
    dof[...] = jnp.zeros((40, EL), f32)
    for q in range(NQ):
        dof[0:NB, q * LN : (q + 1) * LN] = state[q]
    integral[...] = time_step * dof[...]
    matrix = stiffness_rows(stiffness, pad, False)

    def degree(n, weight):
        couple(spread, dof, coupled)
        current = -dot3(matrix, coupled[...])
        dof[...] = current
        weight = weight * time_step / (n + 2).astype(f32)
        integral[...] = integral[...] + weight * current
        return weight

    lax.fori_loop(0, 4, degree, jnp.float32(time_step))
    faces = face_rows(projection, pad)
    trace[...] = dot3(faces[0:64, 0:40], integral[...])
    index[...] = jnp.zeros((8, LN), jnp.int32)
    index[0:6, 0:16] = send[...]
    lane = lax.broadcasted_iota(jnp.int32, (8, LN), 1)
    wanted = jnp.zeros((8, LN), jnp.int32)
    for spot, direction in enumerate((1, 0, 3, 2, 5, 4)):
        row = jnp.broadcast_to(index[direction : direction + 1, :], (8, LN))
        row = pltpu.roll(row, 16 * spot, 1) if spot else row
        wanted = jnp.where(lane // 16 == spot, row, wanted)
    wanted = jnp.concatenate([wanted, wanted], axis=0)
    for q in range(NQ):
        sent[:, q * LN : (q + 1) * LN] = pick(
            lambda s: trace[s * 16 : (s + 1) * 16, q * LN : (q + 1) * LN],
            wanted & 127, wanted >> 7, 4,
        )
    sent[:, EL:] = jnp.zeros((16, TILE), f32)
    sent[0:1, EL:] = east[0:1, :]
    sent[1:2, EL:] = east[TILE - 1 : TILE, :]
    sent[2:3, EL:] = as_row(north[:, 0:1])
    sent[3:4, EL:] = as_row(north[:, TILE - 1 : TILE])
    couple(spread, integral, coupled)
    volume = dot3(stiffness_rows(stiffness, pad, True), coupled[...])
    base[...] = volume
    for q in range(NQ):
        base[0:NB, q * LN : (q + 1) * LN] = volume[0:NB, q * LN : (q + 1) * LN] + state[q]


def predict(state, jacobians, stiffness, projection, send, east, north):
    return pl.pallas_call(
        predict_kernel,
        out_shape=(shaped(40, EL), shaped(64, EL), shaped(16, EDGE)),
        scratch_shapes=[
            pltpu.VMEM((243 * 8, LN), f32),
            pltpu.VMEM((40, EL), f32),
            pltpu.VMEM((LN, EL), f32),
            pltpu.VMEM((LN, LN), f32),
            pltpu.VMEM((8, LN), jnp.int32),
            pltpu.VMEM((40, EL), f32),
        ],
        compiler_params=limit(24),
        cost_estimate=cost(4),
        name="predict",
    )(state, jacobians, stiffness, projection, send, east, north)


def choose_kernel(trace, floor, out):
    def tile(r, carry):
        face = jnp.broadcast_to(floor[pl.ds(r, 1), :], (16, LN))
        out[r] = pick(
            lambda s: trace[s * 16 : (s + 1) * 16, 8 * LN : 9 * LN], face & 127, face >> 7, 4
        )
        return carry

    lax.fori_loop(0, floor.shape[0], tile, 0, unroll=8)


def choose(trace, floor):
    return pl.pallas_call(
        choose_kernel,
        out_shape=shaped(floor.shape[0], NF + 1, LN),
        compiler_params=limit(16),
        cost_estimate=cost(2),
        name="choose",
    )(trace, floor)


def uplift_kernel(inbound, chosen, heights, out):
    for r in range(heights.shape[0]):
        out[r, 0:1, :] = jnp.sum(inbound[r] * chosen[r], axis=0, keepdims=True)
        out[r, 1:2, :] = heights[r : r + 1, :]


def uplift(inbound, chosen, heights):
    return pl.pallas_call(
        uplift_kernel,
        out_shape=shaped(heights.shape[0], 2, LN),
        compiler_params=limit(16),
        cost_estimate=cost(1),
        name="uplift",
    )(inbound, chosen, heights)


def pressure_kernel(inbound, landed, floor, load, left, right):
    zero = jnp.zeros((16, LN), bf16)
    one = jnp.ones((16, LN), bf16)

    def chunk(c, total):
        for i in range(8):
            r = c * 8 + i
            face = floor[pl.ds(r, 1), :]
            high, low = split(inbound[r] * landed[r, 1:2, :])
            (right[i],) = one_hot(face & 127, LN, [one])
            side = jnp.broadcast_to((face >> 7).astype(f32), (16, LN)).astype(bf16)
            for f in range(4):
                hit = side == jnp.full((16, LN), f, bf16)
                left[i, f * 16 : (f + 1) * 16] = jnp.where(hit, high, zero)
                left[i, 64 + f * 16 : 64 + (f + 1) * 16] = jnp.where(hit, low, zero)
        return total + joined(left, right)

    total = lax.fori_loop(0, floor.shape[0] // 8, chunk, jnp.zeros((LN, LN), f32))
    load[...] = total[:64] + total[64:]


def pressure(inbound, landed, floor):
    return pl.pallas_call(
        pressure_kernel,
        out_shape=shaped(64, LN),
        scratch_shapes=[pltpu.VMEM((8, LN, LN), bf16), pltpu.VMEM((8, LN, LN), bf16)],
        compiler_params=limit(16),
        cost_estimate=cost(3),
        name="pressure",
    )(inbound, landed, floor)


def flux_kernel(
    meta, state, base, load, trace, below_x, above_x, below_y, above_y, below_z, above_z,
    source, own, other, projection, mask, out, numeric, received, pad,
):
    faces = face_rows(projection, pad)
    matrix = faces[...].T[0:40, 0:64]
    lane = lax.broadcasted_iota(jnp.int32, (16, LN), 1)
    sides = (
        (below_x, meta[1] > 0), (above_x, meta[1] < meta[4] - 1),
        (below_y, meta[2] > 0), (above_y, meta[2] < meta[5] - 1),
        (below_z, meta[0] > 0), (above_z, meta[0] < meta[3] - 1),
    )
    low = [jnp.where(there, 16 * n, LN) for n, (_, there) in enumerate(sides)]
    for q in range(NQ):
        here = slice(q * LN, (q + 1) * LN)
        found = jnp.zeros((16, LN), f32)
        for n, (side, _) in enumerate(sides):
            hit = (lane >= low[n]) & (lane < low[n] + 16)
            found = jnp.where(hit, side[:, here], found)
        received[:, here] = found

    for f in range(4):
        which = jnp.broadcast_to(source[f : f + 1, :], (16, LN))
        rows = slice(f * 16, (f + 1) * 16)
        total = [None] * NQ
        for q in range(NQ):
            here = slice(q * LN, (q + 1) * LN)
            mine = trace[rows, here]
            remote = pick(
                lambda s: received[:, here] if s == 4 else trace[s * 16 : (s + 1) * 16, here],
                which & 127, which >> 7, 5,
            )
            for p in range(NQ):
                term = mine * own[q, p, f : f + 1, :] + remote * other[q, p, f : f + 1, :]
                total[p] = term if total[p] is None else total[p] + term
        for p in range(NQ):
            numeric[rows, p * LN : (p + 1) * LN] = total[p]
    numeric[:, 2 * LN : 3 * LN] = numeric[:, 2 * LN : 3 * LN] + load[...]
    taken = dot3(matrix, numeric[...])
    updated = base[...] - taken
    live = mask[...] > 0
    for p in range(NQ):
        out[p] = jnp.where(live, updated[0:NB, p * LN : (p + 1) * LN], state[p])


def flux(meta, state, base, load, trace, received, source, own, other, projection, mask):
    smem = pl.BlockSpec(memory_space=pltpu.SMEM)
    vmem = pl.BlockSpec(memory_space=pltpu.VMEM)
    return pl.pallas_call(
        flux_kernel,
        out_shape=shaped(NQ, NB, LN),
        in_specs=[smem] + [vmem] * 15,
        out_specs=vmem,
        scratch_shapes=[
            pltpu.VMEM((64, EL), f32),
            pltpu.VMEM((16, EL), f32),
            pltpu.VMEM((LN, LN), f32),
        ],
        compiler_params=limit(16),
        cost_estimate=cost(4),
        name="flux",
    )(meta, state, base, load, trace, *received, source, own, other, projection, mask)


def ocean_kernel(
    meta, first, second, third, fourth, cell, below_x, above_x, below_y, above_y,
    height, east, north, depth, new_height, edges, total, lifts,
):
    layers = meta[3]
    per = first.shape[0]
    total[...] = jnp.zeros((2 * TILE, TILE), f32)
    one = jnp.ones((16, LN), bf16)
    for shift, values in enumerate((first, second, third, fourth)):
        layer = lax.rem(meta[0] - shift + layers, layers)
        lifts[pl.ds(pl.multiple_of(layer * per, 8), per)] = values[:, 0, :]

    def chunk(c, carry):
        for half in range(2):
            t = c * 2 + half
            cells = cell[0, :, pl.ds(pl.multiple_of(t * LN, LN), LN)]
            for pair in range(2):
                left, right = [], []
                for layer in (2 * pair, 2 * pair + 1):
                    here = cells[layer : layer + 1, :]
                    value = jnp.broadcast_to(lifts[pl.ds(layer * per + t, 1), :], (16, LN))
                    left.append(jnp.concatenate(one_hot(here >> 8, TILE, split(value)), axis=0))
                    right += one_hot(here & 255, TILE, [one])
                total[...] += lax.dot_general(
                    jnp.concatenate(left, axis=1), jnp.concatenate(right, axis=1), NT,
                    preferred_element_type=f32,
                )
        return carry

    lax.fori_loop(0, per // 2, chunk, 0, unroll=8)
    source = total[0:TILE] + total[TILE:]
    rim = slice(EL, EDGE)
    low_x = jnp.where(meta[1] > 0, below_x[1:2, rim], 0.0)
    high_x = jnp.where(meta[1] < meta[4] - 1, above_x[0:1, rim], 0.0)
    low_y = as_column(jnp.where(meta[2] > 0, below_y[3:4, rim], 0.0))
    high_y = as_column(jnp.where(meta[2] < meta[5] - 1, above_y[2:3, rim], 0.0))
    slope = neighbours(east[...], low_x, high_x) * 0.5
    slope = slope + neighbours_lanes(north[...], low_y, high_y) * 0.5
    updated = height[...] + ocean_step * (source - depth[...] * slope)
    new_height[...] = updated
    edges[...] = jnp.zeros((8, TILE), f32)
    edges[0:1] = updated[0:1, :]
    edges[1:2] = updated[TILE - 1 : TILE, :]
    edges[2:3] = as_row(updated[:, 0:1])
    edges[3:4] = as_row(updated[:, TILE - 1 : TILE])


def ocean(meta, layers, cell, received, height, east, north, depth):
    smem = pl.BlockSpec(memory_space=pltpu.SMEM)
    vmem = pl.BlockSpec(memory_space=pltpu.VMEM)
    return pl.pallas_call(
        ocean_kernel,
        out_shape=(shaped(TILE, TILE), shaped(8, TILE)),
        in_specs=[smem] + [vmem] * 13,
        out_specs=(vmem, vmem),
        scratch_shapes=[
            pltpu.VMEM((2 * TILE, TILE), f32),
            pltpu.VMEM((4 * layers[0].shape[0], LN), f32),
        ],
        compiler_params=limit(32),
        cost_estimate=cost(10),
        name="ocean",
    )(meta, *layers, cell, *received[:4], height, east, north, depth)


def flow_kernel(meta, height, east, north, below_x, above_x, below_y, above_y, new_east, new_north):
    low_x = jnp.where(meta[1] > 0, below_x[1:2], 0.0)
    high_x = jnp.where(meta[1] < meta[4] - 1, above_x[0:1], 0.0)
    low_y = as_column(jnp.where(meta[2] > 0, below_y[3:4], 0.0))
    high_y = as_column(jnp.where(meta[2] < meta[5] - 1, above_y[2:3], 0.0))
    level = height[...]
    new_east[...] = east[...] - ocean_step * neighbours(level, low_x, high_x) * 0.5
    new_north[...] = north[...] - ocean_step * neighbours_lanes(level, low_y, high_y) * 0.5


def flow(meta, height, east, north, received):
    smem = pl.BlockSpec(memory_space=pltpu.SMEM)
    vmem = pl.BlockSpec(memory_space=pltpu.VMEM)
    return pl.pallas_call(
        flow_kernel,
        out_shape=(shaped(TILE, TILE), shaped(TILE, TILE)),
        in_specs=[smem] + [vmem] * 7,
        out_specs=(vmem, vmem),
        compiler_params=limit(16),
        cost_estimate=cost(2),
        name="flow",
    )(meta, height, east, north, *received)


def shifted(value, axis, step):
    count = lax.axis_size(axis)
    return lax.ppermute(value, axis, [(i, (i + step) % count) for i in range(count)])


def on_device(
    element_state,
    jacobians,
    stiffness,
    projection,
    flux_self,
    flux_other,
    face_source,
    send_faces,
    cluster_mask,
    seafloor_face,
    ocean_cell,
    ocean_weight,
    height,
    east_flow,
    north_flow,
    water_depth,
):
    names = ("gz", "gx", "gy")
    spot = jnp.arange(8, dtype=jnp.int32)
    meta = jnp.zeros((8,), jnp.int32)
    for n, axis in enumerate(names):
        meta = jnp.where(spot == n, lax.axis_index(axis).astype(jnp.int32), meta)
        meta = jnp.where(spot == n + 3, lax.axis_size(axis), meta)
    floor = seafloor_face.reshape(-1, LN)
    mask = cluster_mask.reshape(1, LN)
    jacobians, flux_self, flux_other = (
        jnp.transpose(x, (1, 2, 0, 3)) for x in (jacobians, flux_self, flux_other)
    )
    projection = jnp.transpose(projection, (1, 0, 2))
    weight = jnp.transpose(ocean_weight, (0, 2, 1, 3))
    inbound = lax.all_to_all(arrange(meta, weight), ("gx", "gy"), 0, 0, tiled=True)
    base, trace, sent = predict(
        element_state, jacobians, stiffness, projection, send_faces, east_flow, north_flow
    )
    heights = lookup(meta, ocean_cell, height)
    early = [shifted(sent, "gz", step) for step in (1, -1)]
    chosen = choose(trace, floor)
    inbound, chosen, heights, *early = lax.optimization_barrier((inbound, chosen, heights, *early))
    lifted = uplift(inbound, chosen, heights)
    landed = lax.all_to_all(lifted, ("gx", "gy"), 0, 0, tiled=True)
    received = [shifted(sent, axis, step) for axis in ("gx", "gy") for step in (1, -1)] + early
    layers = [landed] + [shifted(landed, "gz", step) for step in (1, 2, 3)]
    load = pressure(inbound, landed, floor)
    new_height, edges = ocean(
        meta, layers, ocean_cell, received, height, east_flow, north_flow, water_depth
    )
    rims = [shifted(edges, axis, step) for axis in ("gx", "gy") for step in (1, -1)]
    next_state = flux(
        meta, element_state, base, load, trace, received, face_source, flux_self, flux_other,
        projection, mask,
    )
    new_east, new_north = flow(meta, new_height, east_flow, north_flow, rims)
    return (next_state, new_height, new_east, new_north)


def solution(mesh):
    return jax.shard_map(
        on_device,
        mesh=mesh,
        in_specs=(
            P(None, None, ("gx", "gy", "gz")),
            P(None, None, None, ("gx", "gy", "gz")),
            P(),
            P(),
            P(None, None, None, ("gx", "gy", "gz")),
            P(None, None, None, ("gx", "gy", "gz")),
            P(None, ("gx", "gy", "gz")),
            P(None, ("gx", "gy", "gz")),
            P(("gx", "gy", "gz")),
            P(("gx", "gy", "gz")),
            P(("gx", "gy"), None, None),
            P(("gx", "gy"), None, None, None),
            P("gx", "gy"),
            P("gx", "gy"),
            P("gx", "gy"),
            P("gx", "gy"),
        ),
        out_specs=(P(None, None, ("gx", "gy", "gz")), P("gx", "gy"), P("gx", "gy"), P("gx", "gy")),
        check_vma=False,
    )
```

```python
import jax
import jax.numpy as jnp
from jax import lax
from jax.experimental import pallas as pl
from jax.experimental.pallas import tpu as pltpu
from jax.sharding import PartitionSpec as P

NQ = 9
NB = 35
NF = 15
LN = 128
EL = NQ * LN
TILE = 256
SLAB = 1024
WIDE = 2048
EDGE = EL + TILE

time_step = 1.5
ocean_step = 0.5
f32 = jnp.float32
bf16 = jnp.bfloat16
NT = (((1,), (1,)), ((), ()))


def cost(us):
    return pl.CostEstimate(flops=int(us * 2e8), bytes_accessed=1 << 20, transcendentals=0)


def limit(mib):
    return pltpu.CompilerParams(vmem_limit_bytes=mib << 20)


def shaped(*dims):
    return jax.ShapeDtypeStruct(dims, f32)


def split(x):
    high = x.astype(bf16)
    return high, (x - high.astype(f32)).astype(bf16)


def dot3(left, right):
    rows = left.shape[0]
    left_high, left_low = split(left)
    right_high, right_low = split(right)
    both = jnp.dot(
        jnp.concatenate([left_high, left_low], axis=0), right_high, preferred_element_type=f32
    )
    return both[:rows] + both[rows:] + jnp.dot(left_high, right_low, preferred_element_type=f32)


def block(q):
    return pl.ds(q * LN, LN)


def one_hot(row, count, value):
    lanes = row.shape[1]
    target = jnp.broadcast_to(row.astype(f32), (16, lanes)).astype(bf16)
    ids = lax.broadcasted_iota(jnp.int32, (16, lanes), 0).astype(f32)
    zero = jnp.zeros((16, lanes), bf16)
    hits = [target == (ids + 16.0 * c).astype(bf16) for c in range(count // 16)]
    return [jnp.concatenate([jnp.where(h, v, zero) for h in hits], axis=0) for v in value]


def joined(left, right):
    whole = [jnp.concatenate([r[i] for i in range(8)], axis=1) for r in (left, right)]
    return lax.dot_general(*whole, NT, preferred_element_type=f32)


def pick(table, index, which, sources):
    found = jnp.zeros(index.shape, f32)
    for s in range(sources):
        taken = jnp.take_along_axis(table(s), index, axis=1)
        found = jnp.where(which == s, taken, found)
    return found


def as_row(column):
    size = column.shape[0]
    eye = lax.broadcasted_iota(jnp.int32, (size, size), 0) == lax.broadcasted_iota(
        jnp.int32, (size, size), 1
    )
    return jnp.sum(jnp.where(eye, column, 0.0), axis=0, keepdims=True)


def as_column(row):
    size = row.shape[1]
    eye = lax.broadcasted_iota(jnp.int32, (size, size), 0) == lax.broadcasted_iota(
        jnp.int32, (size, size), 1
    )
    return jnp.sum(jnp.where(eye, row, 0.0), axis=1, keepdims=True)


def neighbours(x, low_row, high_row):
    size = x.shape[0]
    ids = lax.broadcasted_iota(jnp.int32, x.shape, 0)
    after = jnp.where(ids == size - 1, high_row, pltpu.roll(x, size - 1, 0))
    before = jnp.where(ids == 0, low_row, pltpu.roll(x, 1, 0))
    return after - before


def neighbours_lanes(x, low_col, high_col):
    size = x.shape[1]
    ids = lax.broadcasted_iota(jnp.int32, x.shape, 1)
    after = jnp.where(ids == size - 1, high_col, pltpu.roll(x, size - 1, 1))
    before = jnp.where(ids == 0, low_col, pltpu.roll(x, 1, 1))
    return after - before


def arrange_kernel(meta, weight, out):
    for n in range(weight.shape[2]):

        @pl.when(meta[0] == n)
        def _():
            for t in range(WIDE // LN):
                for a in range(NF):
                    out[t, a : a + 1, :] = weight[0, a, n : n + 1, t * LN : (t + 1) * LN]

    out[:, NF : NF + 1, :] = jnp.zeros((WIDE // LN, 1, LN), f32)


def arrange(meta, weight):
    steps = weight.shape[3] // WIDE
    per = WIDE // LN
    return pl.pallas_call(
        arrange_kernel,
        out_shape=shaped(steps * per, NF + 1, LN),
        grid=(steps,),
        in_specs=[
            pl.BlockSpec(memory_space=pltpu.SMEM),
            pl.BlockSpec((1, NF, weight.shape[2], WIDE), lambda s: (0, 0, 0, s)),
        ],
        out_specs=pl.BlockSpec((per, NF + 1, LN), lambda s: (s, 0, 0)),
        compiler_params=limit(60),
        cost_estimate=cost(1),
        name="arrange",
    )(meta, weight)


def lookup_kernel(meta, cell, height, out, high_low):
    high, low = split(height[...])
    high_low[0:TILE] = high
    high_low[TILE:] = low
    layer = meta[0]
    one = jnp.ones((16, TILE), bf16)
    ids = lax.broadcasted_iota(jnp.int32, (TILE, TILE), 0)

    def pair(c, carry):
        for half in range(4):
            t = c * 8 + half * 2
            start = pl.multiple_of(t * LN, TILE)
            cells = cell[0, 0:1, pl.ds(start, TILE)]
            for n in range(1, cell.shape[1]):
                cells = jnp.where(layer == n, cell[0, n : n + 1, pl.ds(start, TILE)], cells)
            rows, cols = (cells >> 8, cells & 255)
            (hot,) = one_hot(cols, TILE, [one])
            both = jnp.dot(high_low[...], hot, preferred_element_type=f32)
            found = both[:TILE] + both[TILE:]
            values = jnp.sum(jnp.where(ids == rows, found, 0.0), axis=0, keepdims=True)
            out[pl.ds(t, 1), :] = values[:, 0:LN]
            out[pl.ds(t + 1, 1), :] = values[:, LN:]
        return carry

    lax.fori_loop(0, out.shape[0] // 8, pair, 0)


def lookup(meta, ocean_cell, height):
    smem = pl.BlockSpec(memory_space=pltpu.SMEM)
    vmem = pl.BlockSpec(memory_space=pltpu.VMEM)
    return pl.pallas_call(
        lookup_kernel,
        out_shape=shaped(ocean_cell.shape[2] // LN, LN),
        in_specs=[smem, vmem, vmem],
        out_specs=vmem,
        scratch_shapes=[pltpu.VMEM((2 * TILE, TILE), bf16)],
        compiler_params=limit(16),
        cost_estimate=cost(6),
        name="lookup",
    )(meta, ocean_cell, height)


def spread_jacobians(jacobians, spread):
    for d in range(3):
        for p in range(NQ):
            for q in range(NQ):
                at = ((d * NQ + p) * NQ + q) * 8
                spread[at : at + 8] = jnp.broadcast_to(jacobians[p, q, d : d + 1, :], (8, LN))


def couple(spread, dof, coupled):
    def rows(b, carry):
        here = pl.ds(pl.multiple_of(b * 8, 8), 8)
        parts = [dof[here, q * LN : (q + 1) * LN] for q in range(NQ)]
        for d in range(3):
            for p in range(NQ):
                total = None
                for q in range(NQ):
                    at = ((d * NQ + p) * NQ + q) * 8
                    term = spread[at : at + 8] * parts[q]
                    total = term if total is None else total + term
                coupled[pl.ds(pl.multiple_of(d * 40 + b * 8, 8), 8), p * LN : (p + 1) * LN] = total
        return carry

    lax.fori_loop(0, 5, rows, 0)


def stiffness_rows(stiffness, pad, transposed):
    total = None
    for d in range(3):
        pad[...] = jnp.zeros((LN, LN), f32)
        pad[0:NB, 0:NB] = stiffness[d]
        value = pad[...].T[0:40] if transposed else pad[0:40]
        value = pltpu.roll(value, d * 40, 1) if d else value
        total = value if total is None else total + value
    return total


def face_rows(projection, pad):
    pad[...] = jnp.zeros((LN, LN), f32)
    for f in range(4):
        for a in range(NF):
            pad[f * 16 + a : f * 16 + a + 1, 0:NB] = projection[a, f : f + 1, :]
    return pad


def predict_kernel(
    state, jacobians, stiffness, projection, send, east, north, base, trace, sent,
    spread, dof, coupled, pad, index, integral,
):
    spread_jacobians(jacobians, spread)
    coupled[...] = jnp.zeros((LN, EL), f32)
    dof[...] = jnp.zeros((40, EL), f32)
    for q in range(NQ):
        dof[0:NB, q * LN : (q + 1) * LN] = state[q]
    integral[...] = time_step * dof[...]
    matrix = stiffness_rows(stiffness, pad, False)

    def degree(n, weight):
        couple(spread, dof, coupled)
        current = -dot3(matrix, coupled[...])
        dof[...] = current
        weight = weight * time_step / (n + 2).astype(f32)
        integral[...] = integral[...] + weight * current
        return weight

    lax.fori_loop(0, 4, degree, jnp.float32(time_step))
    faces = face_rows(projection, pad)
    trace[...] = dot3(faces[0:64, 0:40], integral[...])
    index[...] = jnp.zeros((8, LN), jnp.int32)
    index[0:6, 0:16] = send[...]
    lane = lax.broadcasted_iota(jnp.int32, (8, LN), 1)
    wanted = jnp.zeros((8, LN), jnp.int32)
    for spot, direction in enumerate((1, 0, 3, 2, 5, 4)):
        row = jnp.broadcast_to(index[direction : direction + 1, :], (8, LN))
        row = pltpu.roll(row, 16 * spot, 1) if spot else row
        wanted = jnp.where(lane // 16 == spot, row, wanted)
    wanted = jnp.concatenate([wanted, wanted], axis=0)
    for q in range(NQ):
        sent[:, q * LN : (q + 1) * LN] = pick(
            lambda s: trace[s * 16 : (s + 1) * 16, q * LN : (q + 1) * LN],
            wanted & 127, wanted >> 7, 4,
        )
    sent[:, EL:] = jnp.zeros((16, TILE), f32)
    sent[0:1, EL:] = east[0:1, :]
    sent[1:2, EL:] = east[TILE - 1 : TILE, :]
    sent[2:3, EL:] = as_row(north[:, 0:1])
    sent[3:4, EL:] = as_row(north[:, TILE - 1 : TILE])
    couple(spread, integral, coupled)
    volume = dot3(stiffness_rows(stiffness, pad, True), coupled[...])
    base[...] = volume
    for q in range(NQ):
        base[0:NB, q * LN : (q + 1) * LN] = volume[0:NB, q * LN : (q + 1) * LN] + state[q]


def predict(state, jacobians, stiffness, projection, send, east, north):
    return pl.pallas_call(
        predict_kernel,
        out_shape=(shaped(40, EL), shaped(64, EL), shaped(16, EDGE)),
        scratch_shapes=[
            pltpu.VMEM((243 * 8, LN), f32),
            pltpu.VMEM((40, EL), f32),
            pltpu.VMEM((LN, EL), f32),
            pltpu.VMEM((LN, LN), f32),
            pltpu.VMEM((8, LN), jnp.int32),
            pltpu.VMEM((40, EL), f32),
        ],
        compiler_params=limit(24),
        cost_estimate=cost(4),
        name="predict",
    )(state, jacobians, stiffness, projection, send, east, north)


def choose_kernel(trace, floor, out):
    def tile(r, carry):
        face = jnp.broadcast_to(floor[pl.ds(r, 1), :], (16, LN))
        out[r] = pick(
            lambda s: trace[s * 16 : (s + 1) * 16, 8 * LN : 9 * LN], face & 127, face >> 7, 4
        )
        return carry

    lax.fori_loop(0, floor.shape[0], tile, 0, unroll=8)


def choose(trace, floor):
    return pl.pallas_call(
        choose_kernel,
        out_shape=shaped(floor.shape[0], NF + 1, LN),
        compiler_params=limit(16),
        cost_estimate=cost(2),
        name="choose",
    )(trace, floor)


def uplift_kernel(inbound, chosen, heights, out):
    for r in range(heights.shape[0]):
        out[r, 0:1, :] = jnp.sum(inbound[r] * chosen[r], axis=0, keepdims=True)
        out[r, 1:2, :] = heights[r : r + 1, :]


def uplift(inbound, chosen, heights):
    return pl.pallas_call(
        uplift_kernel,
        out_shape=shaped(heights.shape[0], 2, LN),
        compiler_params=limit(16),
        cost_estimate=cost(1),
        name="uplift",
    )(inbound, chosen, heights)


def pressure_kernel(inbound, landed, floor, load, left, right):
    zero = jnp.zeros((16, LN), bf16)
    one = jnp.ones((16, LN), bf16)

    def chunk(c, total):
        for i in range(8):
            r = c * 8 + i
            face = floor[pl.ds(r, 1), :]
            high, low = split(inbound[r] * landed[r, 1:2, :])
            (right[i],) = one_hot(face & 127, LN, [one])
            side = jnp.broadcast_to((face >> 7).astype(f32), (16, LN)).astype(bf16)
            for f in range(4):
                hit = side == jnp.full((16, LN), f, bf16)
                left[i, f * 16 : (f + 1) * 16] = jnp.where(hit, high, zero)
                left[i, 64 + f * 16 : 64 + (f + 1) * 16] = jnp.where(hit, low, zero)
        return total + joined(left, right)

    total = lax.fori_loop(0, floor.shape[0] // 8, chunk, jnp.zeros((LN, LN), f32), unroll=4)
    load[...] = total[:64] + total[64:]


def pressure(inbound, landed, floor):
    return pl.pallas_call(
        pressure_kernel,
        out_shape=shaped(64, LN),
        scratch_shapes=[pltpu.VMEM((8, LN, LN), bf16), pltpu.VMEM((8, LN, LN), bf16)],
        compiler_params=limit(16),
        cost_estimate=cost(3),
        name="pressure",
    )(inbound, landed, floor)


def flux_kernel(
    meta, state, base, load, trace, below_x, above_x, below_y, above_y, below_z, above_z,
    source, own, other, projection, mask, out, numeric, received, pad,
):
    faces = face_rows(projection, pad)
    matrix = faces[...].T[0:40, 0:64]
    lane = lax.broadcasted_iota(jnp.int32, (16, LN), 1)
    sides = (
        (below_x, meta[1] > 0), (above_x, meta[1] < meta[4] - 1),
        (below_y, meta[2] > 0), (above_y, meta[2] < meta[5] - 1),
        (below_z, meta[0] > 0), (above_z, meta[0] < meta[3] - 1),
    )
    low = [jnp.where(there, 16 * n, LN) for n, (_, there) in enumerate(sides)]
    for q in range(NQ):
        here = slice(q * LN, (q + 1) * LN)
        found = jnp.zeros((16, LN), f32)
        for n, (side, _) in enumerate(sides):
            hit = (lane >= low[n]) & (lane < low[n] + 16)
            found = jnp.where(hit, side[:, here], found)
        received[:, here] = found

    for f in range(4):
        which = jnp.broadcast_to(source[f : f + 1, :], (16, LN))
        rows = slice(f * 16, (f + 1) * 16)
        total = [None] * NQ
        for q in range(NQ):
            here = slice(q * LN, (q + 1) * LN)
            mine = trace[rows, here]
            remote = pick(
                lambda s: received[:, here] if s == 4 else trace[s * 16 : (s + 1) * 16, here],
                which & 127, which >> 7, 5,
            )
            for p in range(NQ):
                term = mine * own[q, p, f : f + 1, :] + remote * other[q, p, f : f + 1, :]
                total[p] = term if total[p] is None else total[p] + term
        for p in range(NQ):
            numeric[rows, p * LN : (p + 1) * LN] = total[p]
    numeric[:, 2 * LN : 3 * LN] = numeric[:, 2 * LN : 3 * LN] + load[...]
    taken = dot3(matrix, numeric[...])
    updated = base[...] - taken
    live = mask[...] > 0
    for p in range(NQ):
        out[p] = jnp.where(live, updated[0:NB, p * LN : (p + 1) * LN], state[p])


def flux(meta, state, base, load, trace, received, source, own, other, projection, mask):
    smem = pl.BlockSpec(memory_space=pltpu.SMEM)
    vmem = pl.BlockSpec(memory_space=pltpu.VMEM)
    return pl.pallas_call(
        flux_kernel,
        out_shape=shaped(NQ, NB, LN),
        in_specs=[smem] + [vmem] * 15,
        out_specs=vmem,
        scratch_shapes=[
            pltpu.VMEM((64, EL), f32),
            pltpu.VMEM((16, EL), f32),
            pltpu.VMEM((LN, LN), f32),
        ],
        compiler_params=limit(16),
        cost_estimate=cost(4),
        name="flux",
    )(meta, state, base, load, trace, *received, source, own, other, projection, mask)


def ocean_kernel(
    meta, first, second, third, fourth, cell, below_x, above_x, below_y, above_y,
    height, east, north, depth, new_height, edges, total, lifts,
):
    layers = meta[3]
    per = first.shape[0]
    total[...] = jnp.zeros((2 * TILE, TILE), f32)
    one = jnp.ones((16, LN), bf16)
    for shift, values in enumerate((first, second, third, fourth)):
        layer = lax.rem(meta[0] - shift + layers, layers)
        lifts[pl.ds(pl.multiple_of(layer * per, 8), per)] = values[:, 0, :]

    def chunk(c, carry):
        for half in range(2):
            t = c * 2 + half
            cells = cell[0, :, pl.ds(pl.multiple_of(t * LN, LN), LN)]
            for pair in range(2):
                left, right = [], []
                for layer in (2 * pair, 2 * pair + 1):
                    here = cells[layer : layer + 1, :]
                    value = jnp.broadcast_to(lifts[pl.ds(layer * per + t, 1), :], (16, LN))
                    left.append(jnp.concatenate(one_hot(here >> 8, TILE, split(value)), axis=0))
                    right += one_hot(here & 255, TILE, [one])
                total[...] += lax.dot_general(
                    jnp.concatenate(left, axis=1), jnp.concatenate(right, axis=1), NT,
                    preferred_element_type=f32,
                )
        return carry

    lax.fori_loop(0, per // 2, chunk, 0, unroll=8)
    source = total[0:TILE] + total[TILE:]
    rim = slice(EL, EDGE)
    low_x = jnp.where(meta[1] > 0, below_x[1:2, rim], 0.0)
    high_x = jnp.where(meta[1] < meta[4] - 1, above_x[0:1, rim], 0.0)
    low_y = as_column(jnp.where(meta[2] > 0, below_y[3:4, rim], 0.0))
    high_y = as_column(jnp.where(meta[2] < meta[5] - 1, above_y[2:3, rim], 0.0))
    slope = neighbours(east[...], low_x, high_x) * 0.5
    slope = slope + neighbours_lanes(north[...], low_y, high_y) * 0.5
    updated = height[...] + ocean_step * (source - depth[...] * slope)
    new_height[...] = updated
    edges[...] = jnp.zeros((8, TILE), f32)
    edges[0:1] = updated[0:1, :]
    edges[1:2] = updated[TILE - 1 : TILE, :]
    edges[2:3] = as_row(updated[:, 0:1])
    edges[3:4] = as_row(updated[:, TILE - 1 : TILE])


def ocean(meta, layers, cell, received, height, east, north, depth):
    smem = pl.BlockSpec(memory_space=pltpu.SMEM)
    vmem = pl.BlockSpec(memory_space=pltpu.VMEM)
    return pl.pallas_call(
        ocean_kernel,
        out_shape=(shaped(TILE, TILE), shaped(8, TILE)),
        in_specs=[smem] + [vmem] * 13,
        out_specs=(vmem, vmem),
        scratch_shapes=[
            pltpu.VMEM((2 * TILE, TILE), f32),
            pltpu.VMEM((4 * layers[0].shape[0], LN), f32),
        ],
        compiler_params=limit(32),
        cost_estimate=cost(10),
        name="ocean",
    )(meta, *layers, cell, *received[:4], height, east, north, depth)


def flow_kernel(meta, height, east, north, below_x, above_x, below_y, above_y, new_east, new_north):
    low_x = jnp.where(meta[1] > 0, below_x[1:2], 0.0)
    high_x = jnp.where(meta[1] < meta[4] - 1, above_x[0:1], 0.0)
    low_y = as_column(jnp.where(meta[2] > 0, below_y[3:4], 0.0))
    high_y = as_column(jnp.where(meta[2] < meta[5] - 1, above_y[2:3], 0.0))
    level = height[...]
    new_east[...] = east[...] - ocean_step * neighbours(level, low_x, high_x) * 0.5
    new_north[...] = north[...] - ocean_step * neighbours_lanes(level, low_y, high_y) * 0.5


def flow(meta, height, east, north, received):
    smem = pl.BlockSpec(memory_space=pltpu.SMEM)
    vmem = pl.BlockSpec(memory_space=pltpu.VMEM)
    return pl.pallas_call(
        flow_kernel,
        out_shape=(shaped(TILE, TILE), shaped(TILE, TILE)),
        in_specs=[smem] + [vmem] * 7,
        out_specs=(vmem, vmem),
        compiler_params=limit(16),
        cost_estimate=cost(2),
        name="flow",
    )(meta, height, east, north, *received)


def shifted(value, axis, step):
    count = lax.axis_size(axis)
    return lax.ppermute(value, axis, [(i, (i + step) % count) for i in range(count)])


def on_device(
    element_state,
    jacobians,
    stiffness,
    projection,
    flux_self,
    flux_other,
    face_source,
    send_faces,
    cluster_mask,
    seafloor_face,
    ocean_cell,
    ocean_weight,
    height,
    east_flow,
    north_flow,
    water_depth,
):
    names = ("gz", "gx", "gy")
    spot = jnp.arange(8, dtype=jnp.int32)
    meta = jnp.zeros((8,), jnp.int32)
    for n, axis in enumerate(names):
        meta = jnp.where(spot == n, lax.axis_index(axis).astype(jnp.int32), meta)
        meta = jnp.where(spot == n + 3, lax.axis_size(axis), meta)
    floor = seafloor_face.reshape(-1, LN)
    mask = cluster_mask.reshape(1, LN)
    jacobians, flux_self, flux_other = (
        jnp.transpose(x, (1, 2, 0, 3)) for x in (jacobians, flux_self, flux_other)
    )
    projection = jnp.transpose(projection, (1, 0, 2))
    weight = jnp.transpose(ocean_weight, (0, 2, 1, 3))
    inbound = lax.all_to_all(arrange(meta, weight), ("gx", "gy"), 0, 0, tiled=True)
    base, trace, sent = predict(
        element_state, jacobians, stiffness, projection, send_faces, east_flow, north_flow
    )
    heights = lookup(meta, ocean_cell, height)
    early = [shifted(sent, "gz", step) for step in (1, -1)]
    chosen = choose(trace, floor)
    inbound, chosen, heights, *early = lax.optimization_barrier((inbound, chosen, heights, *early))
    lifted = uplift(inbound, chosen, heights)
    landed = lax.all_to_all(lifted, ("gx", "gy"), 0, 0, tiled=True)
    received = [shifted(sent, axis, step) for axis in ("gx", "gy") for step in (1, -1)] + early
    layers = [landed] + [shifted(landed, "gz", step) for step in (1, 2, 3)]
    load = pressure(inbound, landed, floor)
    new_height, edges = ocean(
        meta, layers, ocean_cell, received, height, east_flow, north_flow, water_depth
    )
    rims = [shifted(edges, axis, step) for axis in ("gx", "gy") for step in (1, -1)]
    next_state = flux(
        meta, element_state, base, load, trace, received, face_source, flux_self, flux_other,
        projection, mask,
    )
    new_east, new_north = flow(meta, new_height, east_flow, north_flow, rims)
    return (next_state, new_height, new_east, new_north)


def solution(mesh):
    return jax.shard_map(
        on_device,
        mesh=mesh,
        in_specs=(
            P(None, None, ("gx", "gy", "gz")),
            P(None, None, None, ("gx", "gy", "gz")),
            P(),
            P(),
            P(None, None, None, ("gx", "gy", "gz")),
            P(None, None, None, ("gx", "gy", "gz")),
            P(None, ("gx", "gy", "gz")),
            P(None, ("gx", "gy", "gz")),
            P(("gx", "gy", "gz")),
            P(("gx", "gy", "gz")),
            P(("gx", "gy"), None, None),
            P(("gx", "gy"), None, None, None),
            P("gx", "gy"),
            P("gx", "gy"),
            P("gx", "gy"),
            P("gx", "gy"),
        ),
        out_specs=(P(None, None, ("gx", "gy", "gz")), P("gx", "gy"), P("gx", "gy"), P("gx", "gy")),
        check_vma=False,
    )
```
